32 devices in a mesh: azim: 16 (over z, y, core), rad: 2 (over x).
Axes of the slice: x: 2, y: 2, z: 4, core: 2. Of those that a mesh axis runs over, the one named last changes fastest.
Arguments:
- acoustic_state: float32 [5, 128, 32, 128], P(None, 'azim', 'rad'), may hold values from -6 to 6
- mean_flow: float32 [3, 32, 128], P(None, 'rad'), may hold values from -0.5 to 0.5
- sector_offset: int32 [2], replicated, may hold values from 0 to 15
- cell_shift: int32 [2, 128], P(None, 'azim'), may hold values from -3 to 0
- stencil_start: int32 [2, 128], P(None, 'azim'), may hold values from 0 to 1
- interface_fraction: float32 [2, 128], P(None, 'azim'), may hold values from 0 to 1
Outputs:
- next_state: float32 [5, 128, 32, 128], P(None, 'azim', 'rad')
The draws below stay inside these ranges and needn't reach their ends.
All inputs are finite; a program needn't handle non-finite values.
Results may differ from the reference program's by a relative error of at most 0.00005.
Values sent between devices are 32-bit elements; how exact they have to be, the bound alone decides.
A program may use at most 64 MiB of HBM per device.

```python
import jax
import jax.numpy as jnp
from jax import lax

CA = 8
CX = 128
STEPS = 2
NA = 128
NR = 32
N_AZIM = 16


def plant(values, stream_key, least, top_value):
    longest = values.shape.index(max(values.shape))
    spots = []
    for shift in (0, 1):
        where = [jax.random.randint(jax.random.fold_in(stream_key, axis), (), 0, length) for axis, length in enumerate(values.shape)]
        where[longest] = (where[longest] + shift) % values.shape[longest]
        spots.append(tuple(where))
    return values.at[spots[0]].set(least).at[spots[1]].set(top_value)


def levels(own_key, extent, split, smallest, largest):
    def one(axis_at, parts):
        heights = jax.random.uniform(jax.random.fold_in(jax.random.fold_in(own_key, 6), axis_at), (parts,), jnp.float32, smallest / len(split), largest / len(split))
        return jnp.repeat(jnp.exp(heights), extent[axis_at] // parts).reshape((-1,) + (1,) * (len(extent) - axis_at - 1))

    level = one(*split[0])
    for cut in split[1:]:
        level = level * one(*cut)
    return level


def noise(own_key, extent, width, most, cuts=(), kind=jnp.bfloat16):
    entries = jax.random.normal(own_key, extent, jnp.float32) * width
    if len(cuts) > 0:
        entries = levels(own_key, extent, cuts, -0.22, 0.18) * entries
    return jnp.clip(entries, min=-most, max=most).astype(kind)


def setup_inputs(seed: int = 0) -> dict:
    streams_of = jax.random.split(jax.random.key(seed), 7)
    acoustic_state = noise(streams_of[0], (5, NA, NR, CX), 1.0, 6.0, ((1, 16), (2, 2)), jnp.float32)
    mean_flow = jnp.clip(jax.random.uniform(streams_of[1], (3, NR, CX), jnp.float32, -0.5, 0.5) * levels(streams_of[1], (3, NR, CX), ((1, 2),), -0.4, 0.0), -0.5, 0.5)
    sector_offset = jax.random.randint(streams_of[2], (STEPS,), 0, N_AZIM).astype(jnp.int32)
    cell_shift = plant(jax.random.randint(streams_of[3], (STEPS, NA), -3, 1), jax.random.fold_in(streams_of[3], 1), -3, 0).astype(jnp.int32)
    stencil_start = plant(jax.random.randint(streams_of[4], (2, NA), 0, 2), jax.random.fold_in(streams_of[4], 1), 0, 1).astype(jnp.int32)
    interface_fraction = jnp.clip(1.0 * jax.random.uniform(streams_of[5], (2, NA), jnp.float32) ** levels(streams_of[5], (2, NA), ((1, 16),), -0.2, 0.2), 0.0, 1.0)
    return dict(acoustic_state=acoustic_state, mean_flow=mean_flow, sector_offset=sector_offset, cell_shift=cell_shift, stencil_start=stencil_start, interface_fraction=interface_fraction)


STENCIL = (0.841570125482, -0.244678631765, 0.059463584768, -0.007650904064)
STEP_SIZE = 0.2


def derive(extended, along_dim, length):
    summed = None
    for shift_no in range(4):
        forward = lax.slice_in_dim(extended, 5 + shift_no, 5 + shift_no + length, axis=along_dim)
        behind = lax.slice_in_dim(extended, 3 - shift_no, 3 - shift_no + length, axis=along_dim)
        addend = STENCIL[shift_no] * (forward - behind)
        summed = addend if summed is None else summed + addend
    return summed


def lagrange(fraction):
    up_one = fraction + 1.0
    down_one = fraction - 1.0
    down_two = fraction - 2.0
    return jnp.stack([-fraction * down_one * down_two / 6.0, up_one * down_one * down_two / 2.0,
                      -up_one * fraction * down_two / 2.0, up_one * fraction * down_one / 6.0], axis=-1)


def blend(rim_block, first_cell, weights, total_cells):
    summed = jnp.zeros(rim_block.shape, jnp.float32)
    for point_no in range(4):
        source = jnp.mod(first_cell + point_no, total_cells).astype(jnp.int32)
        summed = summed + weights[:, point_no][None, :, None, None] * jnp.take(rim_block, source, axis=1)
    return summed


def evaluate(current, mean_flow, offset, cell_move, stencil_start, interface_fraction):
    total_cells = current.shape[1]
    radial = current.shape[2]
    axial_cells = current.shape[3]
    middle = axial_cells // 2
    beside_all = jnp.concatenate([current[:, -4:], current, current[:, :4]], axis=1)
    beside = jnp.pad(current, ((0, 0), (0, 0), (4, 4), (0, 0)))
    index_cells = jnp.arange(total_cells, dtype=jnp.int32)
    stator_first = index_cells - offset * CA + cell_move + stencil_start[0] - 1
    rotor_first = index_cells + offset * CA - cell_move + stencil_start[1] - 4
    stator_ghost = blend(current[:, :, :, middle:middle + 4], stator_first, lagrange(interface_fraction[0]), total_cells)
    rotor_ghost = blend(current[:, :, :, middle - 4:middle], rotor_first, lagrange(interface_fraction[1]), total_cells)
    zero_pad = jnp.zeros(current.shape[:3] + (4,), jnp.float32)
    stator_line = jnp.concatenate([zero_pad, current[:, :, :, :middle], stator_ghost], axis=3)
    rotor_line = jnp.concatenate([rotor_ghost, current[:, :, :, middle:], zero_pad], axis=3)
    axial_slope = jnp.concatenate([derive(stator_line, 3, middle), derive(rotor_line, 3, axial_cells - middle)], axis=3)
    azim_slope = derive(beside_all, 1, total_cells)
    radial_slope = derive(beside, 2, radial)
    flow_axial = mean_flow[0][None, None]
    flow_radial = mean_flow[1][None, None]
    flow_azim = mean_flow[2][None, None]
    advect = flow_axial * axial_slope + flow_radial * radial_slope + flow_azim * azim_slope
    spread = axial_slope[1] + radial_slope[2] + azim_slope[3]
    forcing = jnp.stack([spread, axial_slope[4], radial_slope[4], azim_slope[4], spread])
    return -advect - forcing


def reference(acoustic_state, mean_flow, sector_offset, cell_shift, stencil_start, interface_fraction):
    current = acoustic_state
    for step_no in range(STEPS):
        offset = sector_offset[step_no]
        cell_move = cell_shift[step_no]
        midpoint = current + (0.5 * STEP_SIZE) * evaluate(current, mean_flow, offset, cell_move, stencil_start, interface_fraction)
        current = current + STEP_SIZE * evaluate(midpoint, mean_flow, offset, cell_move, stencil_start, interface_fraction)
    return current
```

```python
import functools

import jax
import jax.numpy as jnp
from jax import lax
from jax.experimental import pallas as pl
from jax.experimental.pallas import tpu as pltpu
from jax.sharding import PartitionSpec as P

STENCIL = (0.841570125482, -0.244678631765, 0.059463584768, -0.007650904064)
STEP_SIZE = 0.2
MESH = pl.DeviceIdType.MESH
HIGHEST = lax.Precision.HIGHEST
GROUP = 4
RIM = 8
TILE = 8
HALO = 4


def dot(a, b):
    return jnp.dot(a, b, precision=HIGHEST, preferred_element_type=jnp.float32)


def iota(shape, dim):
    return lax.broadcasted_iota(jnp.int32, shape, dim)


def kernel(
    dims,
    q_hbm, flow_hbm, offset_hbm, shift_hbm, start_hbm, fraction_hbm,
    out_ref,
    flow_ref, offset_ref, shift_ref, start_ref, fraction_ref, in_sem,
    cur, azim_halo, rad_send, rad_halo, near, far_send, far, slopes, change, flow_pack, wide, deriv,
    near_held, far_held, near_ssem, near_rsem, far_ssem, far_rsem, azim_ssem, azim_rsem, rad_ssem, rad_rsem,
):
    fields, cells, radial, lanes, steps, n_azim, n_rad = dims
    evals = 2 * steps
    n_high = n_azim // GROUP
    middle = lanes // 2
    low_lane = middle - HALO
    r_tiles = radial // TILE
    me = lax.axis_index("azim")
    rad = lax.axis_index("rad")
    high, low = me // GROUP, lax.rem(me, GROUP)
    left, right = lax.rem(me + n_azim - 1, n_azim), lax.rem(me + 1, n_azim)
    near_peers = [lax.rem(high + i, n_high) for i in range(1, n_high)]
    far_peers = [lax.rem(low + i, GROUP) for i in range(1, GROUP)]

    rows = pl.ds(TILE, radial)
    state_in = pltpu.make_async_copy(q_hbm, cur.at[0, :, :, rows, :], in_sem.at[0])
    state_in.start()
    barrier = pltpu.get_barrier_semaphore()

    def greet(azim_to, rad_to):
        pl.semaphore_signal(barrier, inc=1, device_id=(azim_to, rad_to), device_id_type=MESH)

    for peer in near_peers:
        greet(peer * GROUP + low, rad)
    for peer in far_peers:
        greet(high * GROUP + peer, rad)
    greet(left, rad)
    greet(right, rad)

    @pl.when(rad > 0)
    def _():
        greet(me, rad - 1)

    @pl.when(rad < n_rad - 1)
    def _():
        greet(me, rad + 1)

    small_in = [
        pltpu.make_async_copy(source, target, in_sem.at[1 + i])
        for i, (source, target) in enumerate((
            (flow_hbm, flow_ref), (offset_hbm, offset_ref), (shift_hbm, shift_ref),
            (start_hbm, start_ref), (fraction_hbm, fraction_ref),
        ))
    ]
    for copy in small_in:
        copy.start()

    lane = iota((1, lanes), 1)
    lane_rim = lax.rem(lane, RIM)
    lane_group = lane // RIM
    rotor_side = lane_rim >= HALO
    lane_cell = lane_group // r_tiles

    def packed(piece_of):
        out = None
        for group in range(cells * r_tiles):
            piece = piece_of(group // r_tiles, group % r_tiles)
            turn = (RIM * group - low_lane) % lanes
            piece = pltpu.roll(piece, turn, 1) if turn else piece
            out = piece if out is None else jnp.where(lane_group == group, piece, out)
        return out

    at_interface = (lane >= low_lane) & (lane < low_lane + RIM)

    def unpacked(value, group):
        turn = (low_lane - RIM * group) % lanes
        value = pltpu.roll(value, turn, 1) if turn else value
        return jnp.where(at_interface, value, 0.0)

    def near_copy(e, slot, peer, i):
        return pltpu.make_async_remote_copy(
            src_ref=near.at[e, high], dst_ref=near.at[e, slot],
            send_sem=near_ssem.at[e, i], recv_sem=near_rsem.at[e, slot],
            device_id=(peer * GROUP + low, rad), device_id_type=MESH,
        )

    def far_copy(e, slot, peer, i):
        return pltpu.make_async_remote_copy(
            src_ref=far_send.at[e, i], dst_ref=far.at[e, slot],
            send_sem=far_ssem.at[e, i], recv_sem=far_rsem.at[e, slot],
            device_id=(high * GROUP + peer, rad), device_id_type=MESH,
        )

    def azim_copy(e, side):
        source = cells - HALO if side == 0 else 0
        return pltpu.make_async_remote_copy(
            src_ref=cur.at[e, :, pl.ds(source, HALO), rows, :], dst_ref=azim_halo.at[e, side],
            send_sem=azim_ssem.at[e, side], recv_sem=azim_rsem.at[e, side],
            device_id=(right if side == 0 else left, rad), device_id_type=MESH,
        )

    def rad_copy(e, side):
        return pltpu.make_async_remote_copy(
            src_ref=rad_send.at[e, side], dst_ref=rad_halo.at[e, side],
            send_sem=rad_ssem.at[e, side], recv_sem=rad_rsem.at[e, side],
            device_id=(me, rad + 1 if side == 0 else rad - 1), device_id_type=MESH,
        )

    def add_change(e):
        for f in range(fields):
            value = change[f]
            for group in range(cells * r_tiles):
                a, t = group // r_tiles, group % r_tiles
                spot = pl.ds(TILE * (t + 1), TILE)
                cur[e, f, a, spot, :] += unpacked(value, group)

    def send_rims(e):
        for i, peer in enumerate(near_peers):
            near_copy(e, high, peer, i).start()

    def send_halos(e):
        for side in range(2):
            azim_copy(e, side).start()

        @pl.when(rad < n_rad - 1)
        def _():
            rad_send[e, 0] = cur[e, :, :, pl.ds(TILE + radial - HALO, HALO), :]
            rad_copy(e, 0).start()

        @pl.when(rad > 0)
        def _():
            rad_send[e, 1] = cur[e, :, :, pl.ds(TILE, HALO), :]
            rad_copy(e, 1).start()

    state_in.wait()
    for f in range(fields):
        near[0, high, f] = packed(lambda a, t: cur[0, f, a, pl.ds(TILE * (t + 1), TILE), :])
    beside = jnp.where(rad > 0, 1, 0) + jnp.where(rad < n_rad - 1, 1, 0)
    pl.semaphore_wait(barrier, n_high - 1 + GROUP - 1 + 2 + beside)

    send_rims(0)
    send_halos(0)
    @pl.when(rad == 0)
    def _():
        for e in range(evals):
            rad_halo[e, 0] = jnp.zeros(rad_halo.shape[2:], jnp.float32)

    @pl.when(rad == n_rad - 1)
    def _():
        for e in range(evals):
            rad_halo[e, 1] = jnp.zeros(rad_halo.shape[2:], jnp.float32)

    for copy in small_in:
        copy.wait()
    row_no = iota((lanes, lanes), 0)
    col_no = iota((lanes, lanes), 1)
    axial = jnp.zeros((lanes, lanes), jnp.float32)
    for j in range(4):
        axial = jnp.where(row_no - col_no == j + 1, STENCIL[j], axial)
        axial = jnp.where(col_no - row_no == j + 1, -STENCIL[j], axial)
    deriv[0] = axial
    crossing = (row_no // RIM == col_no // RIM) & (
        (lax.rem(row_no, RIM) >= HALO) != (lax.rem(col_no, RIM) >= HALO)
    )
    cross = jnp.where(crossing, axial, 0.0)
    deriv[1] = cross

    def per_lane(stator_of, rotor_of, kind):
        out = jnp.zeros((1, lanes), kind)
        for a in range(cells):
            out = jnp.where(lane_cell == a, jnp.where(rotor_side, stator_of(a), rotor_of(a)), out)
        return out

    fraction = per_lane(lambda a: fraction_ref[0, a], lambda a: fraction_ref[1, a], jnp.float32)
    up_one, down_one, down_two = fraction + 1.0, fraction - 1.0, fraction - 2.0
    weights = (
        -fraction * down_one * down_two / 6.0,
        up_one * down_one * down_two / 2.0,
        -up_one * fraction * down_two / 2.0,
        up_one * fraction * down_one / 6.0,
    )
    same = (lax.rem(row_no, RIM * r_tiles) == lax.rem(col_no, RIM * r_tiles))
    for n in range(steps):
        first = per_lane(
            lambda a: shift_ref[n, a] + start_ref[0, a] - 1 + a,
            lambda a: start_ref[1, a] - shift_ref[n, a] - 4 + a,
            jnp.int32,
        )
        for d in range(3):
            point = row_no // (RIM * r_tiles) + cells * (d - 1) - first
            blend = jnp.zeros((lanes, lanes), jnp.float32)
            for m in range(4):
                blend = jnp.where(same & (point == m), weights[m], blend)
            wide[n, d] = dot(blend, cross)

    flow_pack[...] = packed(lambda a, t: flow_ref[0, TILE * t : TILE * (t + 1), :])

    def evaluate(e, carry):
        step = e // 2
        half = lax.rem(e, 2)
        scale = jnp.where(half == 0, 0.5 * STEP_SIZE, STEP_SIZE)
        offset = offset_ref[step]
        own = near[e, high].reshape(fields * TILE, lanes)
        own_cross = dot(own, deriv[1])
        for f in range(fields):
            block = cur[e, f, :, rows, :].reshape(cells * radial, lanes)
            slopes[f] = dot(block, deriv[0]).reshape(cells, radial, lanes)

        for i, peer in enumerate(near_peers):
            near_copy(e, peer, peer, i).wait_recv()
        near_held[...] = near[e]

        def needed(by, holder, sign):
            base = by + sign * offset - 1 + 2 * n_azim
            sector = base + lax.rem(holder - lax.rem(base, GROUP) + GROUP, GROUP)
            return lax.rem(sector, n_azim) // GROUP

        def chosen(peer):
            by = high * GROUP + peer
            return jnp.where(
                rotor_side[None], near_held[needed(by, low, -1)], near_held[needed(by, low, 1)]
            )

        for i, peer in enumerate(far_peers):
            far_send[e, i] = chosen(peer)
            far_copy(e, low, peer, i).start()
        far[e, low] = chosen(low)

        for side in range(2):
            azim_copy(e, side).wait_recv()

        @pl.when(rad > 0)
        def _():
            rad_copy(e, 0).wait_recv()

        @pl.when(rad < n_rad - 1)
        def _():
            rad_copy(e, 1).wait_recv()

        cur[e, :, :, pl.ds(TILE - HALO, HALO), :] = rad_halo[e, 0]
        cur[e, :, :, pl.ds(TILE + radial, HALO), :] = rad_halo[e, 1]

        def cell_row(f, a):
            if a < 0:
                return azim_halo[e, 0, f, a + HALO]
            if a >= cells:
                return azim_halo[e, 1, f, a - cells]
            return cur[e, f, a, rows, :]

        for a in range(cells):
            along = []
            for f in range(fields):
                azim = rad_slope = None
                for j in range(4):
                    term = STENCIL[j] * (cell_row(f, a + j + 1) - cell_row(f, a - j - 1))
                    azim = term if azim is None else azim + term
                    term = STENCIL[j] * (
                        cur[e, f, a, pl.ds(TILE + j + 1, radial), :]
                        - cur[e, f, a, pl.ds(TILE - j - 1, radial), :]
                    )
                    rad_slope = term if rad_slope is None else rad_slope + term
                along.append((slopes[f, a], rad_slope, azim))
            spread = along[1][0] + along[2][1] + along[3][2]
            forcing = (spread, along[4][0], along[4][1], along[4][2], spread)
            for f in range(fields):
                advect = flow_ref[0] * along[f][0] + flow_ref[1] * along[f][1] + flow_ref[2] * along[f][2]
                cur[e + 1, f, a, rows, :] = cur[e - half, f, a, rows, :] - scale * (advect + forcing[f])

        rims = [
            packed(lambda a, t: cur[e + 1, f, a, pl.ds(TILE * (t + 1), TILE), :]) for f in range(fields)
        ]

        for i, peer in enumerate(far_peers):
            far_copy(e, peer, peer, i).wait_recv()
        far_held[...] = far[e]
        moved = None
        for d in range(3):
            stator_from = lax.rem(me - offset - 1 + d + 2 * n_azim, GROUP)
            rotor_from = lax.rem(me + offset - 1 + d + 2 * n_azim, GROUP)
            facing = jnp.where(rotor_side[None], far_held[stator_from], far_held[rotor_from])
            part = dot(facing.reshape(fields * TILE, lanes), wide[step, d])
            moved = part if moved is None else moved + part
        moved = (moved - own_cross).reshape(fields, TILE, lanes)
        forced = (moved[1], moved[4], None, None, moved[1])
        for f in range(fields):
            total = flow_pack[...] * moved[f]
            if forced[f] is not None:
                total = total + forced[f]
            delta = -scale * total
            change[f] = delta
            near[e + 1, high, f] = rims[f] + delta

        @pl.when(e + 1 < evals)
        def _():
            send_rims(e + 1)
            add_change(e + 1)
            send_halos(e + 1)

        return carry

    lax.fori_loop(0, evals, evaluate, 0)
    for f in range(fields):
        value = change[f]
        for group in range(cells * r_tiles):
            a, t = group // r_tiles, group % r_tiles
            out_ref[f, a, TILE * t : TILE * (t + 1), :] = (
                cur[evals, f, a, pl.ds(TILE * (t + 1), TILE), :] + unpacked(value, group)
            )

    def finish(e, carry):
        for i, peer in enumerate(near_peers):
            near_copy(e, high, peer, i).wait_send()
        for i, peer in enumerate(far_peers):
            far_copy(e, low, peer, i).wait_send()
        for side in range(2):
            azim_copy(e, side).wait_send()

        @pl.when(rad < n_rad - 1)
        def _():
            rad_copy(e, 0).wait_send()

        @pl.when(rad > 0)
        def _():
            rad_copy(e, 1).wait_send()

        return carry

    lax.fori_loop(0, evals, finish, 0)


def solution(mesh):
    n_azim, n_rad = mesh.shape["azim"], mesh.shape["rad"]

    def shards(acoustic_state, mean_flow, sector_offset, cell_shift, stencil_start, interface_fraction):
        fields, cells, radial, lanes = acoustic_state.shape
        steps = sector_offset.shape[0]
        evals = 2 * steps
        n_high = n_azim // GROUP
        dims = (fields, cells, radial, lanes, steps, n_azim, n_rad)
        vmem = pl.BlockSpec(memory_space=pltpu.VMEM)
        f32 = jnp.float32
        dma = pltpu.SemaphoreType.DMA
        return pl.pallas_call(
            functools.partial(kernel, dims),
            out_shape=pltpu.VMEM(acoustic_state.shape, f32),
            in_specs=[pl.BlockSpec(memory_space=pl.ANY)] * 6,
            out_specs=vmem,
            scratch_shapes=[
                pltpu.VMEM(mean_flow.shape, f32),
                pltpu.SMEM(sector_offset.shape, jnp.int32),
                pltpu.SMEM(cell_shift.shape, jnp.int32),
                pltpu.SMEM(stencil_start.shape, jnp.int32),
                pltpu.SMEM(interface_fraction.shape, f32),
                dma((6,)),
                pltpu.VMEM((evals + 1, fields, cells, radial + 2 * TILE, lanes), f32),
                pltpu.VMEM((evals, 2, fields, HALO, radial, lanes), f32),
                pltpu.VMEM((evals, 2, fields, cells, HALO, lanes), f32),
                pltpu.VMEM((evals, 2, fields, cells, HALO, lanes), f32),
                pltpu.VMEM((evals + 1, n_high, fields, TILE, lanes), f32),
                pltpu.VMEM((evals, GROUP - 1, fields, TILE, lanes), f32),
                pltpu.VMEM((evals, GROUP, fields, TILE, lanes), f32),
                pltpu.VMEM((fields, cells, radial, lanes), f32),
                pltpu.VMEM((fields, TILE, lanes), f32),
                pltpu.VMEM((TILE, lanes), f32),
                pltpu.VMEM((steps, 3, lanes, lanes), f32),
                pltpu.VMEM((2, lanes, lanes), f32),
                pltpu.VMEM((n_high, fields, TILE, lanes), f32),
                pltpu.VMEM((GROUP, fields, TILE, lanes), f32),
                dma((evals, n_high)), dma((evals, n_high)),
                dma((evals, GROUP)), dma((evals, GROUP)),
                dma((evals, 2)), dma((evals, 2)),
                dma((evals, 2)), dma((evals, 2)),
            ],
            compiler_params=pltpu.CompilerParams(collective_id=0, has_side_effects=True),
        )(acoustic_state, mean_flow, sector_offset, cell_shift, stencil_start, interface_fraction)

    return jax.shard_map(
        shards,
        mesh=mesh,
        in_specs=(
            P(None, "azim", "rad", None),
            P(None, "rad", None),
            P(),
            P(None, "azim"),
            P(None, "azim"),
            P(None, "azim"),
        ),
        out_specs=P(None, "azim", "rad", None),
        check_vma=False,
    )
```

```python
import functools

import jax
import jax.numpy as jnp
from jax import lax
from jax.experimental import pallas as pl
from jax.experimental.pallas import tpu as pltpu
from jax.sharding import PartitionSpec as P

STENCIL = (0.841570125482, -0.244678631765, 0.059463584768, -0.007650904064)
STEP_SIZE = 0.2
MESH = pl.DeviceIdType.MESH
HIGHEST = lax.Precision.HIGHEST
GROUP = 4
RIM = 8
TILE = 8
HALO = 4


def dot(a, b):
    return jnp.dot(a, b, precision=HIGHEST, preferred_element_type=jnp.float32)


def iota(shape, dim):
    return lax.broadcasted_iota(jnp.int32, shape, dim)


def kernel(
    dims,
    q_hbm, flow_hbm, offset_hbm, shift_hbm, start_hbm, fraction_hbm,
    out_ref,
    flow_ref, offset_ref, shift_ref, start_ref, fraction_ref, in_sem,
    raw, cur, azim_halo, rad_send, rad_halo, tile, side, near, far_send, far, slopes, flow_pack, deriv,
    near_held, far_held, par, par_send, par_far,
    near_ssem, near_rsem, far_ssem, far_rsem, azim_ssem, azim_rsem, rad_ssem, rad_rsem, side_ssem, side_rsem,
    par_ssem, par_rsem, pfar_ssem, pfar_rsem,
):
    fields, cells, radial, lanes, steps, n_azim, n_rad = dims
    evals = 2 * steps
    n_high = n_azim // GROUP
    middle = lanes // 2
    low_lane = middle - HALO
    r_tiles = radial // TILE
    span = RIM * r_tiles
    me = lax.axis_index("azim")
    rad = lax.axis_index("rad")
    high, low = me // GROUP, lax.rem(me, GROUP)
    left, right = lax.rem(me + n_azim - 1, n_azim), lax.rem(me + 1, n_azim)
    near_peers = [lax.rem(high + i, n_high) for i in range(1, n_high)]
    far_peers = [lax.rem(low + i, GROUP) for i in range(1, GROUP)]

    rows = pl.ds(TILE, radial)
    state_in = pltpu.make_async_copy(q_hbm, raw.at[0], in_sem.at[0])
    state_in.start()
    barrier = pltpu.get_barrier_semaphore()

    def greet(azim_to, rad_to):
        pl.semaphore_signal(barrier, inc=1, device_id=(azim_to, rad_to), device_id_type=MESH)

    greet(left, rad)
    greet(right, rad)
    for peer in near_peers:
        greet(peer * GROUP + low, rad)
    for peer in far_peers:
        greet(high * GROUP + peer, rad)

    @pl.when(rad > 0)
    def _():
        greet(me, rad - 1)

    @pl.when(rad < n_rad - 1)
    def _():
        greet(me, rad + 1)

    small_in = [
        pltpu.make_async_copy(source, target, in_sem.at[1 + i])
        for i, (source, target) in enumerate((
            (flow_hbm, flow_ref), (offset_hbm, offset_ref), (shift_hbm, shift_ref),
            (start_hbm, start_ref), (fraction_hbm, fraction_ref),
        ))
    ]
    for copy in small_in:
        copy.start()

    shape = (TILE, lanes)
    lane = iota(shape, 1)
    line = iota(shape, 0)
    lane_rim = lax.rem(lane, RIM)
    lane_group = lane // RIM
    rotor_side = lane_rim >= HALO
    lane_cell = lane // span
    lane_tile = lax.rem(lane_group, r_tiles)
    at_interface = (lane >= low_lane) & (lane < low_lane + RIM)

    def roll(value, turn, axis=1):
        turn = turn % value.shape[axis]
        return pltpu.roll(value, turn, axis) if turn else value

    def packed(piece_of):
        out = None
        for group in range(cells * r_tiles):
            piece = roll(piece_of(group // r_tiles, group % r_tiles), RIM * group - low_lane)
            out = piece if out is None else jnp.where(lane_group == group, piece, out)
        return out

    def near_copy(e, slot, peer, i):
        return pltpu.make_async_remote_copy(
            src_ref=near.at[e, high], dst_ref=near.at[e, slot],
            send_sem=near_ssem.at[e, i], recv_sem=near_rsem.at[e, slot],
            device_id=(peer * GROUP + low, rad), device_id_type=MESH,
        )

    def far_copy(e, slot, peer, i):
        return pltpu.make_async_remote_copy(
            src_ref=far_send.at[e, i], dst_ref=far.at[e, slot],
            send_sem=far_ssem.at[e, i], recv_sem=far_rsem.at[e, slot],
            device_id=(high * GROUP + peer, rad), device_id_type=MESH,
        )

    def par_copy(slot, peer, i):
        return pltpu.make_async_remote_copy(
            src_ref=par.at[high], dst_ref=par.at[slot],
            send_sem=par_ssem.at[i], recv_sem=par_rsem.at[slot],
            device_id=(peer * GROUP + low, rad), device_id_type=MESH,
        )

    def pfar_copy(slot, peer, i):
        return pltpu.make_async_remote_copy(
            src_ref=par_send.at[i], dst_ref=par_far.at[slot],
            send_sem=pfar_ssem.at[i], recv_sem=pfar_rsem.at[slot],
            device_id=(high * GROUP + peer, rad), device_id_type=MESH,
        )

    def azim_copy(e, side_no):
        source = cells - HALO if side_no == 0 else 0
        return pltpu.make_async_remote_copy(
            src_ref=raw.at[e, :, pl.ds(source, HALO)], dst_ref=azim_halo.at[e, side_no],
            send_sem=azim_ssem.at[e, side_no], recv_sem=azim_rsem.at[e, side_no],
            device_id=(right if side_no == 0 else left, rad), device_id_type=MESH,
        )

    def rad_copy(e, side_no):
        return pltpu.make_async_remote_copy(
            src_ref=rad_send.at[e, side_no], dst_ref=rad_halo.at[e, side_no],
            send_sem=rad_ssem.at[e, side_no], recv_sem=rad_rsem.at[e, side_no],
            device_id=(me, rad + 1 if side_no == 0 else rad - 1), device_id_type=MESH,
        )

    def side_copy(e, slot):
        target = ((right, rad), (left, rad), (me, rad + 1), (me, rad - 1))[slot]
        return pltpu.make_async_remote_copy(
            src_ref=tile.at[e], dst_ref=side.at[e, slot],
            send_sem=side_ssem.at[e, slot], recv_sem=side_rsem.at[e, slot],
            device_id=target, device_id_type=MESH,
        )

    def on_rad(up, down):
        @pl.when(rad < n_rad - 1)
        def _():
            up()

        @pl.when(rad > 0)
        def _():
            down()

    def send_near(e):
        for i, peer in enumerate(near_peers):
            near_copy(e, high, peer, i).start()

    def send_sides(e):
        side_copy(e, 0).start()
        side_copy(e, 1).start()
        on_rad(lambda: side_copy(e, 2).start(), lambda: side_copy(e, 3).start())

    def wait_sides(e):
        on_rad(lambda: side_copy(e, 3).wait_recv(), lambda: side_copy(e, 2).wait_recv())
        side_copy(e, 0).wait_recv()
        side_copy(e, 1).wait_recv()

    def send_halos(e):
        for side_no in range(2):
            azim_copy(e, side_no).start()

        def up():
            rad_send[e, 0] = raw[e, :, :, pl.ds(radial - HALO, HALO), :]
            rad_copy(e, 0).start()

        def down():
            rad_send[e, 1] = raw[e, :, :, pl.ds(0, HALO), :]
            rad_copy(e, 1).start()

        on_rad(up, down)

    state_in.wait()
    for f in range(fields):
        first_tile = packed(lambda a, t: raw[0, f, a, TILE * t : TILE * (t + 1), :])
        tile[0, f] = first_tile
        near[0, high, f] = first_tile

    for copy in small_in:
        copy.wait()

    def per_lane(on_rotor, on_stator):
        out = jnp.zeros(shape, jnp.float32)
        for a in range(cells):
            out = jnp.where(lane_cell == a, jnp.where(rotor_side, on_rotor(a), on_stator(a)), out)
        return out

    def real(value):
        return value.astype(jnp.float32)

    def stator_first(n):
        return lambda a: real(shift_ref[n, a] + start_ref[0, a] - 1)

    def rotor_first(n):
        return lambda a: real(start_ref[1, a] - shift_ref[n, a] - 4)

    stator_fraction, rotor_fraction = (lambda a: fraction_ref[0, a]), (lambda a: fraction_ref[1, a])
    held = per_lane(rotor_fraction, stator_fraction)
    for n in range(steps):
        held = jnp.where(line == n + 1, per_lane(rotor_first(n), stator_first(n)), held)
    par[high] = held

    beside = jnp.where(rad > 0, 1, 0) + jnp.where(rad < n_rad - 1, 1, 0)
    pl.semaphore_wait(barrier, n_high - 1 + GROUP - 1 + 2 + beside)

    send_near(0)
    send_sides(0)
    send_halos(0)
    for i, peer in enumerate(near_peers):
        par_copy(high, peer, i).start()

    @pl.when(rad == 0)
    def _():
        for e in range(evals):
            rad_halo[e, 0] = jnp.zeros(rad_halo.shape[2:], jnp.float32)
            side[e, 2] = jnp.zeros(side.shape[2:], jnp.float32)

    @pl.when(rad == n_rad - 1)
    def _():
        for e in range(evals):
            rad_halo[e, 1] = jnp.zeros(rad_halo.shape[2:], jnp.float32)
            side[e, 3] = jnp.zeros(side.shape[2:], jnp.float32)

    row_no = iota((lanes, lanes), 0)
    col_no = iota((lanes, lanes), 1)
    axial = jnp.zeros((lanes, lanes), jnp.float32)
    for j in range(4):
        axial = jnp.where(row_no - col_no == j + 1, STENCIL[j], axial)
        axial = jnp.where(col_no - row_no == j + 1, -STENCIL[j], axial)
    deriv[...] = axial
    for i in range(3):
        flow_pack[i] = packed(lambda a, t: flow_ref[i, TILE * t : TILE * (t + 1), :])

    def taps(fraction, first):
        up_one, down_one, down_two = fraction + 1.0, fraction - 1.0, fraction - 2.0
        weights = (
            -fraction * down_one * down_two / 6.0,
            up_one * down_one * down_two / 2.0,
            -up_one * fraction * down_two / 2.0,
            up_one * fraction * down_one / 6.0,
        )
        out = []
        for delta in range(-HALO, HALO):
            tap = jnp.zeros(shape, jnp.float32)
            for m in range(4):
                tap = jnp.where(first == float(delta - m), weights[m], tap)
            out.append(tap)
        return out

    def shifted(before, here, after, delta):
        if delta < 0:
            here = jnp.where(lane_cell >= cells + delta, before, here)
        elif delta > 0:
            here = jnp.where(lane_cell < delta, after, here)
        return roll(here, -span * delta)

    def blend(before, here, after, tap):
        out = None
        for delta in range(-HALO, HALO):
            term = tap[delta + HALO] * shifted(before, here, after, delta)
            out = term if out is None else out + term
        return out

    ahead = [jnp.where((lane_rim < HALO) & (lane_rim + j + 1 >= HALO), STENCIL[j], 0.0) for j in range(4)]
    behind = [jnp.where((lane_rim >= HALO) & (lane_rim - j - 1 < HALO), STENCIL[j], 0.0) for j in range(4)]

    def cross(value):
        out = None
        for j in range(4):
            term = ahead[j] * roll(value, -(j + 1)) - behind[j] * roll(value, j + 1)
            out = term if out is None else out + term
        return out

    def azim_slope(before, here, after):
        out = None
        for j in range(4):
            term = STENCIL[j] * (
                shifted(before, here, after, j + 1) - shifted(before, here, after, -(j + 1))
            )
            out = term if out is None else out + term
        return out

    def radial_slope(below, here, above):
        last = r_tiles - 1
        following = jnp.where(lane_tile == last, roll(above, RIM * last), roll(here, -RIM))
        leading = jnp.where(lane_tile == 0, roll(below, -RIM * last), roll(here, RIM))
        out = None
        for j in range(1, 5):
            up = roll(jnp.where(line >= j, here, following), -j, 0)
            down = roll(jnp.where(line < TILE - j, here, leading), j, 0)
            term = STENCIL[j - 1] * (up - down)
            out = term if out is None else out + term
        return out

    def across(value):
        along = [cross(value[f]) for f in range(fields)]
        forcing = (along[1], along[4], None, None, along[1])
        out = []
        for f in range(fields):
            total = flow_pack[0] * along[f]
            out.append(total if forcing[f] is None else total + forcing[f])
        return out

    def swapped(value):
        return jnp.where(rotor_side, roll(value, HALO), roll(value, -HALO))

    def sector_of(n, by, holder, sign):
        base = by + sign * offset_ref[n] - 1 + 2 * n_azim
        sector = base + lax.rem(holder - lax.rem(base, GROUP) + GROUP, GROUP)
        return lax.rem(sector, n_azim) // GROUP

    def facing_of(n, d):
        offset = offset_ref[n]
        stator_from = lax.rem(me - offset - 1 + d + 2 * n_azim, GROUP)
        rotor_from = lax.rem(me + offset - 1 + d + 2 * n_azim, GROUP)
        return stator_from, rotor_from

    def relay(e, n):
        for i, peer in enumerate(near_peers):
            near_copy(e, peer, peer, i).wait_recv()
        near_held[...] = near[e]

        def chosen(peer):
            by = high * GROUP + peer
            return jnp.where(
                rotor_side[None], near_held[sector_of(n, by, low, -1)], near_held[sector_of(n, by, low, 1)]
            )

        for i, peer in enumerate(far_peers):
            far_send[e, i] = chosen(peer)
            far_copy(e, low, peer, i).start()
        far[e, low] = chosen(low)

    def relay_params():
        for i, peer in enumerate(near_peers):
            par_copy(peer, peer, i).wait_recv()

        def chosen(peer, n):
            by = high * GROUP + peer
            return jnp.where(
                rotor_side, par[sector_of(n, by, low, -1)], par[sector_of(n, by, low, 1)]
            )

        for i, peer in enumerate(far_peers):
            for n in range(steps):
                par_send[i, n] = chosen(peer, n)
            pfar_copy(low, peer, i).start()
        for n in range(steps):
            par_far[low, n] = chosen(low, n)

    def ghosts(e, n, tap):
        for i, peer in enumerate(far_peers):
            far_copy(e, peer, peer, i).wait_recv()
        far_held[...] = far[e]
        spots = [facing_of(n, d) for d in range(3)]
        out = []
        for f in range(fields):
            facing = [jnp.where(rotor_side, far_held[s, f], far_held[r, f]) for s, r in spots]
            out.append(blend(facing[0], facing[1], facing[2], tap))
        return out

    def merge(e):
        for f in range(fields):
            value = tile[e, f]
            for group in range(cells * r_tiles):
                a, t = group // r_tiles, group % r_tiles
                spot = roll(value, low_lane - RIM * group)
                cur[e, f, a, pl.ds(TILE * (t + 1), TILE), :] = jnp.where(
                    at_interface, spot, raw[e, f, a, TILE * t : TILE * (t + 1), :]
                )

    def axial_slopes(e):
        for f in range(fields):
            block = cur[e, f, :, rows, :].reshape(cells * radial, lanes)
            slopes[f] = dot(block, deriv[...]).reshape(cells, radial, lanes)
        out = []
        for f in range(fields):
            plain = packed(lambda a, t: slopes[f, a, TILE * t : TILE * (t + 1), :])
            out.append(plain - cross(tile[e, f]))
        return out

    def rim_state(e, base, scale, along):
        out = []
        slope = []
        for f in range(fields):
            here = tile[e, f]
            slope.append((
                along[f],
                radial_slope(side[e, 2, f], here, side[e, 3, f]),
                azim_slope(side[e, 0, f], here, side[e, 1, f]),
            ))
        spread = slope[1][0] + slope[2][1] + slope[3][2]
        forcing = (spread, slope[4][0], slope[4][1], slope[4][2], spread)
        for f in range(fields):
            advect = flow_pack[0] * slope[f][0] + flow_pack[1] * slope[f][1] + flow_pack[2] * slope[f][2]
            out.append(tile[base, f] - scale * (advect + forcing[f]))
        return out

    def bulk_local(e, base, scale):
        on_rad(lambda: rad_copy(e, 1).wait_recv(), lambda: rad_copy(e, 0).wait_recv())
        cur[e, :, :, pl.ds(TILE - HALO, HALO), :] = rad_halo[e, 0]
        cur[e, :, :, pl.ds(TILE + radial, HALO), :] = rad_halo[e, 1]
        for a in range(cells):
            along = []
            for f in range(fields):
                rad_slope = None
                for j in range(4):
                    term = STENCIL[j] * (
                        cur[e, f, a, pl.ds(TILE + j + 1, radial), :]
                        - cur[e, f, a, pl.ds(TILE - j - 1, radial), :]
                    )
                    rad_slope = term if rad_slope is None else rad_slope + term
                along.append((slopes[f, a], rad_slope))
            spread = along[1][0] + along[2][1]
            forcing = (spread, along[4][0], along[4][1], None, spread)
            for f in range(fields):
                total = flow_ref[0] * along[f][0] + flow_ref[1] * along[f][1]
                if forcing[f] is not None:
                    total = total + forcing[f]
                slopes[f, a] = cur[base, f, a, rows, :] - scale * total

    def bulk_azim(e, scale):
        for side_no in range(2):
            azim_copy(e, side_no).wait_recv()

        def cell_row(f, a):
            if a < 0:
                return azim_halo[e, 0, f, a + HALO]
            if a >= cells:
                return azim_halo[e, 1, f, a - cells]
            return cur[e, f, a, rows, :]

        for a in range(cells):
            along = []
            for f in range(fields):
                azim = None
                for j in range(4):
                    term = STENCIL[j] * (cell_row(f, a + j + 1) - cell_row(f, a - j - 1))
                    azim = term if azim is None else azim + term
                along.append(azim)
            forcing = (along[3], None, None, along[4], along[3])
            for f in range(fields):
                total = flow_ref[2] * along[f]
                if forcing[f] is not None:
                    total = total + forcing[f]
                raw[e + 1, f, a] = slopes[f, a] - scale * total

    half_step = 0.5 * STEP_SIZE

    def advance(n, carry):
        e = 2 * n
        n_row = n + 1
        tap = taps(
            per_lane(stator_fraction, rotor_fraction), per_lane(stator_first(n), rotor_first(n))
        )
        merge(e)
        along = axial_slopes(e)
        relay(e, n)
        wait_sides(e)
        midway = rim_state(e, e, half_step, along)
        for f in range(fields):
            near[e + 1, high, f] = midway[f]
        send_near(e + 1)
        bulk_local(e, e, half_step)

        @pl.when(n == 0)
        def _():
            relay_params()

        bulk_azim(e, half_step)
        send_halos(e + 1)
        push = across(ghosts(e, n, tap))
        for f in range(fields):
            tile[e + 1, f] = midway[f] - half_step * push[f]
        send_sides(e + 1)

        @pl.when(n == 0)
        def _():
            for i, peer in enumerate(far_peers):
                pfar_copy(peer, peer, i).wait_recv()

        merge(e + 1)
        along = axial_slopes(e + 1)

        other = []
        for d in range(3):
            stator_from, rotor_from = facing_of(n, d)
            there = jnp.where(rotor_side, par_far[stator_from, n], par_far[rotor_from, n])
            there = swapped(there)
            fraction = jnp.broadcast_to(there[0:1], shape)
            first = jnp.zeros(shape, jnp.float32)
            for i in range(steps):
                first = jnp.where(n == i, jnp.broadcast_to(there[i + 1 : i + 2], shape), first)
            other.append(taps(fraction, first))
        back = taps(
            per_lane(rotor_fraction, stator_fraction), per_lane(rotor_first(n), stator_first(n))
        )
        twice = []
        for f in range(fields):
            before, here, after = side[e, 0, f], tile[e, f], side[e, 1, f]
            twice.append(blend(
                blend(before, before, here, other[0]),
                blend(before, here, after, other[1]),
                blend(here, after, after, other[2]),
                back,
            ))
        mutual = across(twice)

        relay(e + 1, n)
        bulk_local(e + 1, e, STEP_SIZE)
        wait_sides(e + 1)
        final = rim_state(e + 1, e, STEP_SIZE, along)
        ghost = ghosts(e + 1, n, tap)
        push = across([ghost[f] - half_step * mutual[f] for f in range(fields)])
        for f in range(fields):
            tile[e + 2, f] = final[f] - STEP_SIZE * push[f]

        @pl.when(n + 1 < steps)
        def _():
            for f in range(fields):
                near[e + 2, high, f] = tile[e + 2, f]
            send_near(e + 2)
            send_sides(e + 2)

        bulk_azim(e + 1, STEP_SIZE)

        @pl.when(n + 1 < steps)
        def _():
            send_halos(e + 2)

        return carry

    lax.fori_loop(0, steps, advance, 0)
    for f in range(fields):
        value = tile[evals, f]
        for group in range(cells * r_tiles):
            a, t = group // r_tiles, group % r_tiles
            out_ref[f, a, TILE * t : TILE * (t + 1), :] = jnp.where(
                at_interface, roll(value, low_lane - RIM * group),
                raw[evals, f, a, TILE * t : TILE * (t + 1), :],
            )

    def finish(e, carry):
        for i, peer in enumerate(near_peers):
            near_copy(e, high, peer, i).wait_send()
        for i, peer in enumerate(far_peers):
            far_copy(e, low, peer, i).wait_send()
        for side_no in range(2):
            azim_copy(e, side_no).wait_send()
            side_copy(e, side_no).wait_send()

        def up():
            rad_copy(e, 0).wait_send()
            side_copy(e, 2).wait_send()

        def down():
            rad_copy(e, 1).wait_send()
            side_copy(e, 3).wait_send()

        on_rad(up, down)
        return carry

    lax.fori_loop(0, evals, finish, 0)
    for i, peer in enumerate(near_peers):
        par_copy(high, peer, i).wait_send()
    for i, peer in enumerate(far_peers):
        pfar_copy(low, peer, i).wait_send()


def solution(mesh):
    n_azim, n_rad = mesh.shape["azim"], mesh.shape["rad"]

    def shards(acoustic_state, mean_flow, sector_offset, cell_shift, stencil_start, interface_fraction):
        fields, cells, radial, lanes = acoustic_state.shape
        steps = sector_offset.shape[0]
        evals = 2 * steps
        n_high = n_azim // GROUP
        dims = (fields, cells, radial, lanes, steps, n_azim, n_rad)
        vmem = pl.BlockSpec(memory_space=pltpu.VMEM)
        f32 = jnp.float32
        dma = pltpu.SemaphoreType.DMA
        return pl.pallas_call(
            functools.partial(kernel, dims),
            out_shape=pltpu.VMEM(acoustic_state.shape, f32),
            in_specs=[pl.BlockSpec(memory_space=pl.ANY)] * 6,
            out_specs=vmem,
            scratch_shapes=[
                pltpu.VMEM(mean_flow.shape, f32),
                pltpu.SMEM(sector_offset.shape, jnp.int32),
                pltpu.SMEM(cell_shift.shape, jnp.int32),
                pltpu.SMEM(stencil_start.shape, jnp.int32),
                pltpu.SMEM(interface_fraction.shape, f32),
                dma((6,)),
                pltpu.VMEM((evals + 1, fields, cells, radial, lanes), f32),
                pltpu.VMEM((evals, fields, cells, radial + 2 * TILE, lanes), f32),
                pltpu.VMEM((evals, 2, fields, HALO, radial, lanes), f32),
                pltpu.VMEM((evals, 2, fields, cells, HALO, lanes), f32),
                pltpu.VMEM((evals, 2, fields, cells, HALO, lanes), f32),
                pltpu.VMEM((evals + 1, fields, TILE, lanes), f32),
                pltpu.VMEM((evals, 4, fields, TILE, lanes), f32),
                pltpu.VMEM((evals, n_high, fields, TILE, lanes), f32),
                pltpu.VMEM((evals, GROUP - 1, fields, TILE, lanes), f32),
                pltpu.VMEM((evals, GROUP, fields, TILE, lanes), f32),
                pltpu.VMEM((fields, cells, radial, lanes), f32),
                pltpu.VMEM((3, TILE, lanes), f32),
                pltpu.VMEM((lanes, lanes), f32),
                pltpu.VMEM((n_high, fields, TILE, lanes), f32),
                pltpu.VMEM((GROUP, fields, TILE, lanes), f32),
                pltpu.VMEM((n_high, TILE, lanes), f32),
                pltpu.VMEM((GROUP - 1, steps, TILE, lanes), f32),
                pltpu.VMEM((GROUP, steps, TILE, lanes), f32),
                dma((evals, n_high)), dma((evals, n_high)),
                dma((evals, GROUP)), dma((evals, GROUP)),
                dma((evals, 2)), dma((evals, 2)),
                dma((evals, 2)), dma((evals, 2)),
                dma((evals, 4)), dma((evals, 4)),
                dma((n_high,)), dma((n_high,)),
                dma((GROUP,)), dma((GROUP,)),
            ],
            compiler_params=pltpu.CompilerParams(collective_id=0, has_side_effects=True),
        )(acoustic_state, mean_flow, sector_offset, cell_shift, stencil_start, interface_fraction)

    return jax.shard_map(
        shards,
        mesh=mesh,
        in_specs=(
            P(None, "azim", "rad", None),
            P(None, "rad", None),
            P(),
            P(None, "azim"),
            P(None, "azim"),
            P(None, "azim"),
        ),
        out_specs=P(None, "azim", "rad", None),
        check_vma=False,
    )
```

```python
import functools

import jax
import jax.numpy as jnp
from jax import lax
from jax.experimental import pallas as pl
from jax.experimental.pallas import tpu as pltpu
from jax.sharding import PartitionSpec as P

STENCIL = (0.841570125482, -0.244678631765, 0.059463584768, -0.007650904064)
STEP_SIZE = 0.2
MESH = pl.DeviceIdType.MESH
HIGHEST = lax.Precision.HIGHEST
GROUP = 4
RIM = 8
TILE = 8
HALO = 4


def dot(a, b):
    return jnp.dot(a, b, precision=HIGHEST, preferred_element_type=jnp.float32)


def iota(shape, dim):
    return lax.broadcasted_iota(jnp.int32, shape, dim)


def kernel(
    dims,
    q_hbm, flow_hbm, offset_hbm, shift_hbm, start_hbm, fraction_hbm,
    out_ref,
    flow_ref, offset_ref, shift_ref, start_ref, fraction_ref, in_sem,
    raw, cur, azim_halo, rad_send, rad_halo, tile, side, near, far_send, far, slopes, flow_pack, deriv,
    near_held, far_held, par, par_send, par_far,
    near_ssem, near_rsem, far_ssem, far_rsem, azim_ssem, azim_rsem, rad_ssem, rad_rsem, side_ssem, side_rsem,
    par_ssem, par_rsem, pfar_ssem, pfar_rsem,
):
    fields, cells, radial, lanes, steps, n_azim, n_rad = dims
    evals = 2 * steps
    n_high = n_azim // GROUP
    middle = lanes // 2
    low_lane = middle - HALO
    r_tiles = radial // TILE
    span = RIM * r_tiles
    me = lax.axis_index("azim")
    rad = lax.axis_index("rad")
    high, low = me // GROUP, lax.rem(me, GROUP)
    left, right = lax.rem(me + n_azim - 1, n_azim), lax.rem(me + 1, n_azim)
    near_peers = [lax.rem(high + i, n_high) for i in range(1, n_high)]
    far_peers = [lax.rem(low + i, GROUP) for i in range(1, GROUP)]

    rows = pl.ds(TILE, radial)
    state_in = pltpu.make_async_copy(q_hbm, raw.at[0], in_sem.at[0])
    state_in.start()
    barrier = pltpu.get_barrier_semaphore()

    def greet(azim_to, rad_to):
        pl.semaphore_signal(barrier, inc=1, device_id=(azim_to, rad_to), device_id_type=MESH)

    greet(left, rad)
    greet(right, rad)
    for peer in near_peers:
        greet(peer * GROUP + low, rad)
    for peer in far_peers:
        greet(high * GROUP + peer, rad)

    @pl.when(rad > 0)
    def _():
        greet(me, rad - 1)

    @pl.when(rad < n_rad - 1)
    def _():
        greet(me, rad + 1)

    small_in = [
        pltpu.make_async_copy(source, target, in_sem.at[1 + i])
        for i, (source, target) in enumerate((
            (flow_hbm, flow_ref), (offset_hbm, offset_ref), (shift_hbm, shift_ref),
            (start_hbm, start_ref), (fraction_hbm, fraction_ref),
        ))
    ]
    for copy in small_in:
        copy.start()

    shape = (TILE, lanes)
    lane = iota(shape, 1)
    line = iota(shape, 0)
    lane_rim = lax.rem(lane, RIM)
    lane_group = lane // RIM
    rotor_side = lane_rim >= HALO
    lane_cell = lane // span
    lane_tile = lax.rem(lane_group, r_tiles)
    at_interface = (lane >= low_lane) & (lane < low_lane + RIM)

    def roll(value, turn, axis=1):
        turn = turn % value.shape[axis]
        return pltpu.roll(value, turn, axis) if turn else value

    def packed(piece_of):
        out = None
        for group in range(cells * r_tiles):
            piece = roll(piece_of(group // r_tiles, group % r_tiles), RIM * group - low_lane)
            out = piece if out is None else jnp.where(lane_group == group, piece, out)
        return out

    def near_copy(e, slot, peer, i):
        return pltpu.make_async_remote_copy(
            src_ref=near.at[e, high], dst_ref=near.at[e, slot],
            send_sem=near_ssem.at[e, i], recv_sem=near_rsem.at[e, slot],
            device_id=(peer * GROUP + low, rad), device_id_type=MESH,
        )

    def far_copy(e, slot, peer, i):
        return pltpu.make_async_remote_copy(
            src_ref=far_send.at[e, i], dst_ref=far.at[e, slot],
            send_sem=far_ssem.at[e, i], recv_sem=far_rsem.at[e, slot],
            device_id=(high * GROUP + peer, rad), device_id_type=MESH,
        )

    def par_copy(slot, peer, i):
        return pltpu.make_async_remote_copy(
            src_ref=par.at[high], dst_ref=par.at[slot],
            send_sem=par_ssem.at[i], recv_sem=par_rsem.at[slot],
            device_id=(peer * GROUP + low, rad), device_id_type=MESH,
        )

    def pfar_copy(slot, peer, i):
        return pltpu.make_async_remote_copy(
            src_ref=par_send.at[i], dst_ref=par_far.at[slot],
            send_sem=pfar_ssem.at[i], recv_sem=pfar_rsem.at[slot],
            device_id=(high * GROUP + peer, rad), device_id_type=MESH,
        )

    cuts = (0, 3, 5)

    def azim_copy(e, side_no, part):
        source = cells - HALO if side_no == 0 else 0
        some = pl.ds(cuts[part], cuts[part + 1] - cuts[part])
        return pltpu.make_async_remote_copy(
            src_ref=raw.at[e, some, pl.ds(source, HALO)], dst_ref=azim_halo.at[e, side_no, some],
            send_sem=azim_ssem.at[e, side_no, part], recv_sem=azim_rsem.at[e, side_no, part],
            device_id=(right if side_no == 0 else left, rad), device_id_type=MESH,
        )

    def rad_copy(e, side_no):
        return pltpu.make_async_remote_copy(
            src_ref=rad_send.at[e, side_no], dst_ref=rad_halo.at[e, side_no],
            send_sem=rad_ssem.at[e, side_no], recv_sem=rad_rsem.at[e, side_no],
            device_id=(me, rad + 1 if side_no == 0 else rad - 1), device_id_type=MESH,
        )

    def side_copy(e, slot):
        target = ((right, rad), (left, rad), (me, rad + 1), (me, rad - 1))[slot]
        return pltpu.make_async_remote_copy(
            src_ref=tile.at[e], dst_ref=side.at[e, slot],
            send_sem=side_ssem.at[e, slot], recv_sem=side_rsem.at[e, slot],
            device_id=target, device_id_type=MESH,
        )

    def on_rad(up, down):
        @pl.when(rad < n_rad - 1)
        def _():
            up()

        @pl.when(rad > 0)
        def _():
            down()

    def send_near(e):
        for i, peer in enumerate(near_peers):
            near_copy(e, high, peer, i).start()

    def send_sides(e):
        side_copy(e, 0).start()
        side_copy(e, 1).start()
        on_rad(lambda: side_copy(e, 2).start(), lambda: side_copy(e, 3).start())

    def wait_sides(e):
        on_rad(lambda: side_copy(e, 3).wait_recv(), lambda: side_copy(e, 2).wait_recv())
        side_copy(e, 0).wait_recv()
        side_copy(e, 1).wait_recv()

    def send_halos(e, which):
        for part in which:
            for side_no in range(2):
                azim_copy(e, side_no, part).start()
        if 0 not in which:
            return

        def up():
            rad_send[e, 0] = raw[e, :, :, pl.ds(radial - HALO, HALO), :]
            rad_copy(e, 0).start()

        def down():
            rad_send[e, 1] = raw[e, :, :, pl.ds(0, HALO), :]
            rad_copy(e, 1).start()

        on_rad(up, down)

    state_in.wait()
    for f in range(fields):
        first_tile = packed(lambda a, t: raw[0, f, a, TILE * t : TILE * (t + 1), :])
        tile[0, f] = first_tile
        near[0, high, f] = first_tile

    for copy in small_in:
        copy.wait()

    def per_lane(on_rotor, on_stator):
        out = jnp.zeros(shape, jnp.float32)
        for a in range(cells):
            out = jnp.where(lane_cell == a, jnp.where(rotor_side, on_rotor(a), on_stator(a)), out)
        return out

    def real(value):
        return value.astype(jnp.float32)

    def stator_first(n):
        return lambda a: real(shift_ref[n, a] + start_ref[0, a] - 1)

    def rotor_first(n):
        return lambda a: real(start_ref[1, a] - shift_ref[n, a] - 4)

    stator_fraction, rotor_fraction = (lambda a: fraction_ref[0, a]), (lambda a: fraction_ref[1, a])
    held = per_lane(rotor_fraction, stator_fraction)
    for n in range(steps):
        held = jnp.where(line == n + 1, per_lane(rotor_first(n), stator_first(n)), held)
    par[high] = held

    beside = jnp.where(rad > 0, 1, 0) + jnp.where(rad < n_rad - 1, 1, 0)
    pl.semaphore_wait(barrier, n_high - 1 + GROUP - 1 + 2 + beside)

    send_near(0)
    send_sides(0)
    send_halos(0, range(2))
    for i, peer in enumerate(near_peers):
        par_copy(high, peer, i).start()

    @pl.when(rad == 0)
    def _():
        for e in range(evals):
            rad_halo[e, 0] = jnp.zeros(rad_halo.shape[2:], jnp.float32)
            side[e, 2] = jnp.zeros(side.shape[2:], jnp.float32)

    @pl.when(rad == n_rad - 1)
    def _():
        for e in range(evals):
            rad_halo[e, 1] = jnp.zeros(rad_halo.shape[2:], jnp.float32)
            side[e, 3] = jnp.zeros(side.shape[2:], jnp.float32)

    row_no = iota((lanes, lanes), 0)
    col_no = iota((lanes, lanes), 1)
    axial = jnp.zeros((lanes, lanes), jnp.float32)
    for j in range(4):
        axial = jnp.where(row_no - col_no == j + 1, STENCIL[j], axial)
        axial = jnp.where(col_no - row_no == j + 1, -STENCIL[j], axial)
    deriv[...] = axial
    for i in range(3):
        flow_pack[i] = packed(lambda a, t: flow_ref[i, TILE * t : TILE * (t + 1), :])

    def taps(fraction, first):
        up_one, down_one, down_two = fraction + 1.0, fraction - 1.0, fraction - 2.0
        weights = (
            -fraction * down_one * down_two / 6.0,
            up_one * down_one * down_two / 2.0,
            -up_one * fraction * down_two / 2.0,
            up_one * fraction * down_one / 6.0,
        )
        out = []
        for delta in range(-HALO, HALO):
            tap = jnp.zeros(shape, jnp.float32)
            for m in range(4):
                tap = jnp.where(first == float(delta - m), weights[m], tap)
            out.append(tap)
        return out

    def shifted(before, here, after, delta):
        if delta < 0:
            here = jnp.where(lane_cell >= cells + delta, before, here)
        elif delta > 0:
            here = jnp.where(lane_cell < delta, after, here)
        return roll(here, -span * delta)

    def blend(before, here, after, tap):
        out = None
        for delta in range(-HALO, HALO):
            term = tap[delta + HALO] * shifted(before, here, after, delta)
            out = term if out is None else out + term
        return out

    ahead = [jnp.where((lane_rim < HALO) & (lane_rim + j + 1 >= HALO), STENCIL[j], 0.0) for j in range(4)]
    behind = [jnp.where((lane_rim >= HALO) & (lane_rim - j - 1 < HALO), STENCIL[j], 0.0) for j in range(4)]

    def cross(value):
        out = None
        for j in range(4):
            term = ahead[j] * roll(value, -(j + 1)) - behind[j] * roll(value, j + 1)
            out = term if out is None else out + term
        return out

    def azim_slope(before, here, after):
        out = None
        for j in range(4):
            term = STENCIL[j] * (
                shifted(before, here, after, j + 1) - shifted(before, here, after, -(j + 1))
            )
            out = term if out is None else out + term
        return out

    def radial_slope(below, here, above):
        last = r_tiles - 1
        following = jnp.where(lane_tile == last, roll(above, RIM * last), roll(here, -RIM))
        leading = jnp.where(lane_tile == 0, roll(below, -RIM * last), roll(here, RIM))
        out = None
        for j in range(1, 5):
            up = roll(jnp.where(line >= j, here, following), -j, 0)
            down = roll(jnp.where(line < TILE - j, here, leading), j, 0)
            term = STENCIL[j - 1] * (up - down)
            out = term if out is None else out + term
        return out

    def across(value):
        along = [cross(value[f]) for f in range(fields)]
        forcing = (along[1], along[4], None, None, along[1])
        out = []
        for f in range(fields):
            total = flow_pack[0] * along[f]
            out.append(total if forcing[f] is None else total + forcing[f])
        return out

    def swapped(value):
        return jnp.where(rotor_side, roll(value, HALO), roll(value, -HALO))

    def sector_of(n, by, holder, sign):
        base = by + sign * offset_ref[n] - 1 + 2 * n_azim
        sector = base + lax.rem(holder - lax.rem(base, GROUP) + GROUP, GROUP)
        return lax.rem(sector, n_azim) // GROUP

    def facing_of(n, d):
        offset = offset_ref[n]
        stator_from = lax.rem(me - offset - 1 + d + 2 * n_azim, GROUP)
        rotor_from = lax.rem(me + offset - 1 + d + 2 * n_azim, GROUP)
        return stator_from, rotor_from

    def relay(e, n):
        for i, peer in enumerate(near_peers):
            near_copy(e, peer, peer, i).wait_recv()
        near_held[...] = near[e]

        def chosen(peer):
            by = high * GROUP + peer
            return jnp.where(
                rotor_side[None], near_held[sector_of(n, by, low, -1)], near_held[sector_of(n, by, low, 1)]
            )

        for i, peer in enumerate(far_peers):
            far_send[e, i] = chosen(peer)
            far_copy(e, low, peer, i).start()
        far[e, low] = chosen(low)

    def relay_params():
        for i, peer in enumerate(near_peers):
            par_copy(peer, peer, i).wait_recv()

        def chosen(peer, n):
            by = high * GROUP + peer
            return jnp.where(
                rotor_side, par[sector_of(n, by, low, -1)], par[sector_of(n, by, low, 1)]
            )

        for i, peer in enumerate(far_peers):
            for n in range(steps):
                par_send[i, n] = chosen(peer, n)
            pfar_copy(low, peer, i).start()
        for n in range(steps):
            par_far[low, n] = chosen(low, n)

    def ghosts(e, n, tap):
        for i, peer in enumerate(far_peers):
            far_copy(e, peer, peer, i).wait_recv()
        far_held[...] = far[e]
        spots = [facing_of(n, d) for d in range(3)]
        out = []
        for f in range(fields):
            facing = [jnp.where(rotor_side, far_held[s, f], far_held[r, f]) for s, r in spots]
            out.append(blend(facing[0], facing[1], facing[2], tap))
        return out

    def merge(e):
        for f in range(fields):
            value = tile[e, f]
            for group in range(cells * r_tiles):
                a, t = group // r_tiles, group % r_tiles
                spot = roll(value, low_lane - RIM * group)
                cur[e, f, a, pl.ds(TILE * (t + 1), TILE), :] = jnp.where(
                    at_interface, spot, raw[e, f, a, TILE * t : TILE * (t + 1), :]
                )

    def axial_slopes(e):
        for f in range(fields):
            block = cur[e, f, :, rows, :].reshape(cells * radial, lanes)
            slopes[f] = dot(block, deriv[...]).reshape(cells, radial, lanes)
        out = []
        for f in range(fields):
            plain = packed(lambda a, t: slopes[f, a, TILE * t : TILE * (t + 1), :])
            out.append(plain - cross(tile[e, f]))
        return out

    def rim_state(e, base, scale, along):
        out = []
        slope = []
        for f in range(fields):
            here = tile[e, f]
            slope.append((
                along[f],
                radial_slope(side[e, 2, f], here, side[e, 3, f]),
                azim_slope(side[e, 0, f], here, side[e, 1, f]),
            ))
        spread = slope[1][0] + slope[2][1] + slope[3][2]
        forcing = (spread, slope[4][0], slope[4][1], slope[4][2], spread)
        for f in range(fields):
            advect = flow_pack[0] * slope[f][0] + flow_pack[1] * slope[f][1] + flow_pack[2] * slope[f][2]
            out.append(tile[base, f] - scale * (advect + forcing[f]))
        return out

    def bulk_local(e, base, scale):
        on_rad(lambda: rad_copy(e, 1).wait_recv(), lambda: rad_copy(e, 0).wait_recv())
        cur[e, :, :, pl.ds(TILE - HALO, HALO), :] = rad_halo[e, 0]
        cur[e, :, :, pl.ds(TILE + radial, HALO), :] = rad_halo[e, 1]
        for a in range(cells):
            along = []
            for f in range(fields):
                rad_slope = None
                for j in range(4):
                    term = STENCIL[j] * (
                        cur[e, f, a, pl.ds(TILE + j + 1, radial), :]
                        - cur[e, f, a, pl.ds(TILE - j - 1, radial), :]
                    )
                    rad_slope = term if rad_slope is None else rad_slope + term
                along.append((slopes[f, a], rad_slope))
            spread = along[1][0] + along[2][1]
            forcing = (spread, along[4][0], along[4][1], None, spread)
            for f in range(fields):
                total = flow_ref[0] * along[f][0] + flow_ref[1] * along[f][1]
                if forcing[f] is not None:
                    total = total + forcing[f]
                slopes[f, a] = cur[base, f, a, rows, :] - scale * total

    def bulk_azim(e, scale):
        for side_no in range(2):
            for part in range(len(cuts) - 1):
                azim_copy(e, side_no, part).wait_recv()

        def cell_row(f, a):
            if a < 0:
                return azim_halo[e, 0, f, a + HALO]
            if a >= cells:
                return azim_halo[e, 1, f, a - cells]
            return cur[e, f, a, rows, :]

        for a in range(cells):
            along = []
            for f in range(fields):
                azim = None
                for j in range(4):
                    term = STENCIL[j] * (cell_row(f, a + j + 1) - cell_row(f, a - j - 1))
                    azim = term if azim is None else azim + term
                along.append(azim)
            forcing = (along[3], None, None, along[4], along[3])
            for f in range(fields):
                total = flow_ref[2] * along[f]
                if forcing[f] is not None:
                    total = total + forcing[f]
                raw[e + 1, f, a] = slopes[f, a] - scale * total

    half_step = 0.5 * STEP_SIZE

    def advance(n, carry):
        e = 2 * n
        n_row = n + 1
        tap = taps(
            per_lane(stator_fraction, rotor_fraction), per_lane(stator_first(n), rotor_first(n))
        )
        merge(e)
        along = axial_slopes(e)
        relay(e, n)
        wait_sides(e)
        midway = rim_state(e, e, half_step, along)
        for f in range(fields):
            near[e + 1, high, f] = midway[f]
        send_near(e + 1)
        bulk_local(e, e, half_step)

        @pl.when(n == 0)
        def _():
            relay_params()

        bulk_azim(e, half_step)
        send_halos(e + 1, (0,))
        push = across(ghosts(e, n, tap))
        for f in range(fields):
            tile[e + 1, f] = midway[f] - half_step * push[f]
        send_sides(e + 1)

        merge(e + 1)
        along = axial_slopes(e + 1)

        relay(e + 1, n)
        send_halos(e + 1, (1,))
        bulk_local(e + 1, e, STEP_SIZE)
        @pl.when(n == 0)
        def _():
            for i, peer in enumerate(far_peers):
                pfar_copy(peer, peer, i).wait_recv()

        other = []
        for d in range(3):
            stator_from, rotor_from = facing_of(n, d)
            there = jnp.where(rotor_side, par_far[stator_from, n], par_far[rotor_from, n])
            there = swapped(there)
            fraction = jnp.broadcast_to(there[0:1], shape)
            first = jnp.zeros(shape, jnp.float32)
            for i in range(steps):
                first = jnp.where(n == i, jnp.broadcast_to(there[i + 1 : i + 2], shape), first)
            other.append(taps(fraction, first))
        back = taps(
            per_lane(rotor_fraction, stator_fraction), per_lane(rotor_first(n), stator_first(n))
        )
        twice = []
        for f in range(fields):
            before, here, after = side[e, 0, f], tile[e, f], side[e, 1, f]
            twice.append(blend(
                blend(before, before, here, other[0]),
                blend(before, here, after, other[1]),
                blend(here, after, after, other[2]),
                back,
            ))
        mutual = across(twice)

        wait_sides(e + 1)
        final = rim_state(e + 1, e, STEP_SIZE, along)
        ghost = ghosts(e + 1, n, tap)
        push = across([ghost[f] - half_step * mutual[f] for f in range(fields)])
        for f in range(fields):
            tile[e + 2, f] = final[f] - STEP_SIZE * push[f]

        @pl.when(n + 1 < steps)
        def _():
            for f in range(fields):
                near[e + 2, high, f] = tile[e + 2, f]
            send_near(e + 2)
            send_sides(e + 2)

        bulk_azim(e + 1, STEP_SIZE)

        @pl.when(n + 1 < steps)
        def _():
            send_halos(e + 2, range(2))

        return carry

    lax.fori_loop(0, steps, advance, 0)
    for f in range(fields):
        value = tile[evals, f]
        for group in range(cells * r_tiles):
            a, t = group // r_tiles, group % r_tiles
            out_ref[f, a, TILE * t : TILE * (t + 1), :] = jnp.where(
                at_interface, roll(value, low_lane - RIM * group),
                raw[evals, f, a, TILE * t : TILE * (t + 1), :],
            )

    def finish(e, carry):
        for i, peer in enumerate(near_peers):
            near_copy(e, high, peer, i).wait_send()
        for i, peer in enumerate(far_peers):
            far_copy(e, low, peer, i).wait_send()
        for side_no in range(2):
            for part in range(len(cuts) - 1):
                azim_copy(e, side_no, part).wait_send()
            side_copy(e, side_no).wait_send()

        def up():
            rad_copy(e, 0).wait_send()
            side_copy(e, 2).wait_send()

        def down():
            rad_copy(e, 1).wait_send()
            side_copy(e, 3).wait_send()

        on_rad(up, down)
        return carry

    lax.fori_loop(0, evals, finish, 0)
    for i, peer in enumerate(near_peers):
        par_copy(high, peer, i).wait_send()
    for i, peer in enumerate(far_peers):
        pfar_copy(low, peer, i).wait_send()


def solution(mesh):
    n_azim, n_rad = mesh.shape["azim"], mesh.shape["rad"]

    def shards(acoustic_state, mean_flow, sector_offset, cell_shift, stencil_start, interface_fraction):
        fields, cells, radial, lanes = acoustic_state.shape
        steps = sector_offset.shape[0]
        evals = 2 * steps
        n_high = n_azim // GROUP
        dims = (fields, cells, radial, lanes, steps, n_azim, n_rad)
        vmem = pl.BlockSpec(memory_space=pltpu.VMEM)
        f32 = jnp.float32
        dma = pltpu.SemaphoreType.DMA
        return pl.pallas_call(
            functools.partial(kernel, dims),
            out_shape=pltpu.VMEM(acoustic_state.shape, f32),
            in_specs=[pl.BlockSpec(memory_space=pl.ANY)] * 6,
            out_specs=vmem,
            scratch_shapes=[
                pltpu.VMEM(mean_flow.shape, f32),
                pltpu.SMEM(sector_offset.shape, jnp.int32),
                pltpu.SMEM(cell_shift.shape, jnp.int32),
                pltpu.SMEM(stencil_start.shape, jnp.int32),
                pltpu.SMEM(interface_fraction.shape, f32),
                dma((6,)),
                pltpu.VMEM((evals + 1, fields, cells, radial, lanes), f32),
                pltpu.VMEM((evals, fields, cells, radial + 2 * TILE, lanes), f32),
                pltpu.VMEM((evals, 2, fields, HALO, radial, lanes), f32),
                pltpu.VMEM((evals, 2, fields, cells, HALO, lanes), f32),
                pltpu.VMEM((evals, 2, fields, cells, HALO, lanes), f32),
                pltpu.VMEM((evals + 1, fields, TILE, lanes), f32),
                pltpu.VMEM((evals, 4, fields, TILE, lanes), f32),
                pltpu.VMEM((evals, n_high, fields, TILE, lanes), f32),
                pltpu.VMEM((evals, GROUP - 1, fields, TILE, lanes), f32),
                pltpu.VMEM((evals, GROUP, fields, TILE, lanes), f32),
                pltpu.VMEM((fields, cells, radial, lanes), f32),
                pltpu.VMEM((3, TILE, lanes), f32),
                pltpu.VMEM((lanes, lanes), f32),
                pltpu.VMEM((n_high, fields, TILE, lanes), f32),
                pltpu.VMEM((GROUP, fields, TILE, lanes), f32),
                pltpu.VMEM((n_high, TILE, lanes), f32),
                pltpu.VMEM((GROUP - 1, steps, TILE, lanes), f32),
                pltpu.VMEM((GROUP, steps, TILE, lanes), f32),
                dma((evals, n_high)), dma((evals, n_high)),
                dma((evals, GROUP)), dma((evals, GROUP)),
                dma((evals, 2, 2)), dma((evals, 2, 2)),
                dma((evals, 2)), dma((evals, 2)),
                dma((evals, 4)), dma((evals, 4)),
                dma((n_high,)), dma((n_high,)),
                dma((GROUP,)), dma((GROUP,)),
            ],
            compiler_params=pltpu.CompilerParams(collective_id=0, has_side_effects=True),
        )(acoustic_state, mean_flow, sector_offset, cell_shift, stencil_start, interface_fraction)

    return jax.shard_map(
        shards,
        mesh=mesh,
        in_specs=(
            P(None, "azim", "rad", None),
            P(None, "rad", None),
            P(),
            P(None, "azim"),
            P(None, "azim"),
            P(None, "azim"),
        ),
        out_specs=P(None, "azim", "rad", None),
        check_vma=False,
    )
```

```python
import functools

import jax
import jax.numpy as jnp
from jax import lax
from jax.experimental import pallas as pl
from jax.experimental.pallas import tpu as pltpu
from jax.sharding import PartitionSpec as P

STENCIL = (0.841570125482, -0.244678631765, 0.059463584768, -0.007650904064)
STEP_SIZE = 0.2
MESH = pl.DeviceIdType.MESH
HIGHEST = lax.Precision.HIGHEST
GROUP = 4
RIM = 8
TILE = 8
HALO = 4


def dot(a, b):
    return jnp.dot(a, b, precision=HIGHEST, preferred_element_type=jnp.float32)


def iota(shape, dim):
    return lax.broadcasted_iota(jnp.int32, shape, dim)


def kernel(
    dims,
    q_hbm, flow_hbm, offset_hbm, shift_hbm, start_hbm, fraction_hbm,
    out_ref,
    flow_ref, offset_ref, shift_ref, start_ref, fraction_ref, in_sem,
    raw, cur, azim_halo, rad_send, rad_halo, tile, side, near, far_send, far, slopes, flow_pack, deriv,
    near_held, far_held, par, par_send, par_far,
    near_ssem, near_rsem, far_ssem, far_rsem, azim_ssem, azim_rsem, rad_ssem, rad_rsem, side_ssem, side_rsem,
    par_ssem, par_rsem, pfar_ssem, pfar_rsem,
):
    fields, cells, radial, lanes, steps, n_azim, n_rad = dims
    evals = 2 * steps
    n_high = n_azim // GROUP
    middle = lanes // 2
    low_lane = middle - HALO
    r_tiles = radial // TILE
    span = RIM * r_tiles
    me = lax.axis_index("azim")
    rad = lax.axis_index("rad")
    high, low = me // GROUP, lax.rem(me, GROUP)
    left, right = lax.rem(me + n_azim - 1, n_azim), lax.rem(me + 1, n_azim)
    near_peers = [lax.rem(high + i, n_high) for i in range(1, n_high)]
    far_peers = [lax.rem(low + i, GROUP) for i in range(1, GROUP)]

    rows = pl.ds(TILE, radial)
    state_in = pltpu.make_async_copy(q_hbm, raw.at[0], in_sem.at[0])
    state_in.start()
    barrier = pltpu.get_barrier_semaphore()

    def greet(azim_to, rad_to):
        pl.semaphore_signal(barrier, inc=1, device_id=(azim_to, rad_to), device_id_type=MESH)

    greet(left, rad)
    greet(right, rad)
    for peer in near_peers:
        greet(peer * GROUP + low, rad)
    for peer in far_peers:
        greet(high * GROUP + peer, rad)

    @pl.when(rad > 0)
    def _():
        greet(me, rad - 1)

    @pl.when(rad < n_rad - 1)
    def _():
        greet(me, rad + 1)

    small_in = [
        pltpu.make_async_copy(source, target, in_sem.at[1 + i])
        for i, (source, target) in enumerate((
            (flow_hbm, flow_ref), (offset_hbm, offset_ref), (shift_hbm, shift_ref),
            (start_hbm, start_ref), (fraction_hbm, fraction_ref),
        ))
    ]
    for copy in small_in:
        copy.start()

    shape = (TILE, lanes)
    lane = iota(shape, 1)
    line = iota(shape, 0)
    lane_rim = lax.rem(lane, RIM)
    lane_group = lane // RIM
    rotor_side = lane_rim >= HALO
    lane_cell = lane // span
    lane_tile = lax.rem(lane_group, r_tiles)
    at_interface = (lane >= low_lane) & (lane < low_lane + RIM)

    def roll(value, turn, axis=1):
        turn = turn % value.shape[axis]
        return pltpu.roll(value, turn, axis) if turn else value

    def packed(piece_of):
        out = None
        for group in range(cells * r_tiles):
            piece = roll(piece_of(group // r_tiles, group % r_tiles), RIM * group - low_lane)
            out = piece if out is None else jnp.where(lane_group == group, piece, out)
        return out

    def near_copy(e, slot, peer, i):
        return pltpu.make_async_remote_copy(
            src_ref=near.at[e, high], dst_ref=near.at[e, slot],
            send_sem=near_ssem.at[e, i], recv_sem=near_rsem.at[e, slot],
            device_id=(peer * GROUP + low, rad), device_id_type=MESH,
        )

    def far_copy(e, slot, peer, i):
        return pltpu.make_async_remote_copy(
            src_ref=far_send.at[e, i], dst_ref=far.at[e, slot],
            send_sem=far_ssem.at[e, i], recv_sem=far_rsem.at[e, slot],
            device_id=(high * GROUP + peer, rad), device_id_type=MESH,
        )

    def par_copy(slot, peer, i):
        return pltpu.make_async_remote_copy(
            src_ref=par.at[high], dst_ref=par.at[slot],
            send_sem=par_ssem.at[i], recv_sem=par_rsem.at[slot],
            device_id=(peer * GROUP + low, rad), device_id_type=MESH,
        )

    def pfar_copy(slot, peer, i):
        return pltpu.make_async_remote_copy(
            src_ref=par_send.at[i], dst_ref=par_far.at[slot],
            send_sem=pfar_ssem.at[i], recv_sem=pfar_rsem.at[slot],
            device_id=(high * GROUP + peer, rad), device_id_type=MESH,
        )

    cuts = (0, 3, 5)

    def azim_copy(e, side_no, part):
        source = cells - HALO if side_no == 0 else 0
        some = pl.ds(cuts[part], cuts[part + 1] - cuts[part])
        return pltpu.make_async_remote_copy(
            src_ref=raw.at[e, some, pl.ds(source, HALO)], dst_ref=azim_halo.at[e, side_no, some],
            send_sem=azim_ssem.at[e, side_no, part], recv_sem=azim_rsem.at[e, side_no, part],
            device_id=(right if side_no == 0 else left, rad), device_id_type=MESH,
        )

    def rad_copy(e, side_no):
        return pltpu.make_async_remote_copy(
            src_ref=rad_send.at[e, side_no], dst_ref=rad_halo.at[e, side_no],
            send_sem=rad_ssem.at[e, side_no], recv_sem=rad_rsem.at[e, side_no],
            device_id=(me, rad + 1 if side_no == 0 else rad - 1), device_id_type=MESH,
        )

    def side_copy(e, slot):
        target = ((right, rad), (left, rad), (me, rad + 1), (me, rad - 1))[slot]
        return pltpu.make_async_remote_copy(
            src_ref=tile.at[e], dst_ref=side.at[e, slot],
            send_sem=side_ssem.at[e, slot], recv_sem=side_rsem.at[e, slot],
            device_id=target, device_id_type=MESH,
        )

    def on_rad(up, down):
        @pl.when(rad < n_rad - 1)
        def _():
            up()

        @pl.when(rad > 0)
        def _():
            down()

    def send_near(e):
        for i, peer in enumerate(near_peers):
            near_copy(e, high, peer, i).start()

    def send_sides(e):
        side_copy(e, 0).start()
        side_copy(e, 1).start()
        on_rad(lambda: side_copy(e, 2).start(), lambda: side_copy(e, 3).start())

    def wait_sides(e):
        on_rad(lambda: side_copy(e, 3).wait_recv(), lambda: side_copy(e, 2).wait_recv())
        side_copy(e, 0).wait_recv()
        side_copy(e, 1).wait_recv()

    def send_halos(e, which):
        for part in which:
            for side_no in range(2):
                azim_copy(e, side_no, part).start()
        if 0 not in which:
            return

        def up():
            rad_send[e, 0] = raw[e, :, :, pl.ds(radial - HALO, HALO), :]
            rad_copy(e, 0).start()

        def down():
            rad_send[e, 1] = raw[e, :, :, pl.ds(0, HALO), :]
            rad_copy(e, 1).start()

        on_rad(up, down)

    state_in.wait()
    for f in range(fields):
        first_tile = packed(lambda a, t: raw[0, f, a, TILE * t : TILE * (t + 1), :])
        tile[0, f] = first_tile
        near[0, high, f] = first_tile

    for copy in small_in:
        copy.wait()

    def per_lane(on_rotor, on_stator):
        out = jnp.zeros(shape, jnp.float32)
        for a in range(cells):
            out = jnp.where(lane_cell == a, jnp.where(rotor_side, on_rotor(a), on_stator(a)), out)
        return out

    def real(value):
        return value.astype(jnp.float32)

    def stator_first(n):
        return lambda a: real(shift_ref[n, a] + start_ref[0, a] - 1)

    def rotor_first(n):
        return lambda a: real(start_ref[1, a] - shift_ref[n, a] - 4)

    stator_fraction, rotor_fraction = (lambda a: fraction_ref[0, a]), (lambda a: fraction_ref[1, a])
    held = per_lane(rotor_fraction, stator_fraction)
    for n in range(steps):
        held = jnp.where(line == n + 1, per_lane(rotor_first(n), stator_first(n)), held)
    par[high] = held

    beside = jnp.where(rad > 0, 1, 0) + jnp.where(rad < n_rad - 1, 1, 0)
    pl.semaphore_wait(barrier, n_high - 1 + GROUP - 1 + 2 + beside)

    send_near(0)
    send_sides(0)
    send_halos(0, range(2))
    for i, peer in enumerate(near_peers):
        par_copy(high, peer, i).start()

    @pl.when(rad == 0)
    def _():
        for e in range(evals):
            rad_halo[e, 0] = jnp.zeros(rad_halo.shape[2:], jnp.float32)
            side[e, 2] = jnp.zeros(side.shape[2:], jnp.float32)

    @pl.when(rad == n_rad - 1)
    def _():
        for e in range(evals):
            rad_halo[e, 1] = jnp.zeros(rad_halo.shape[2:], jnp.float32)
            side[e, 3] = jnp.zeros(side.shape[2:], jnp.float32)

    row_no = iota((lanes, lanes), 0)
    col_no = iota((lanes, lanes), 1)
    axial = jnp.zeros((lanes, lanes), jnp.float32)
    for j in range(4):
        axial = jnp.where(row_no - col_no == j + 1, STENCIL[j], axial)
        axial = jnp.where(col_no - row_no == j + 1, -STENCIL[j], axial)
    deriv[...] = axial
    for i in range(3):
        flow_pack[i] = packed(lambda a, t: flow_ref[i, TILE * t : TILE * (t + 1), :])

    def taps(fraction, first):
        up_one, down_one, down_two = fraction + 1.0, fraction - 1.0, fraction - 2.0
        weights = (
            -fraction * down_one * down_two / 6.0,
            up_one * down_one * down_two / 2.0,
            -up_one * fraction * down_two / 2.0,
            up_one * fraction * down_one / 6.0,
        )
        out = []
        for delta in range(-HALO, HALO):
            tap = jnp.zeros(shape, jnp.float32)
            for m in range(4):
                tap = jnp.where(first == float(delta - m), weights[m], tap)
            out.append(tap)
        return out

    def shifted(before, here, after, delta):
        if delta < 0:
            here = jnp.where(lane_cell >= cells + delta, before, here)
        elif delta > 0:
            here = jnp.where(lane_cell < delta, after, here)
        return roll(here, -span * delta)

    def blend(before, here, after, tap):
        out = None
        for delta in range(-HALO, HALO):
            term = tap[delta + HALO] * shifted(before, here, after, delta)
            out = term if out is None else out + term
        return out

    ahead = [jnp.where((lane_rim < HALO) & (lane_rim + j + 1 >= HALO), STENCIL[j], 0.0) for j in range(4)]
    behind = [jnp.where((lane_rim >= HALO) & (lane_rim - j - 1 < HALO), STENCIL[j], 0.0) for j in range(4)]

    def cross(value):
        out = None
        for j in range(4):
            term = ahead[j] * roll(value, -(j + 1)) - behind[j] * roll(value, j + 1)
            out = term if out is None else out + term
        return out

    def azim_slope(before, here, after):
        out = None
        for j in range(4):
            term = STENCIL[j] * (
                shifted(before, here, after, j + 1) - shifted(before, here, after, -(j + 1))
            )
            out = term if out is None else out + term
        return out

    def radial_slope(below, here, above):
        last = r_tiles - 1
        following = jnp.where(lane_tile == last, roll(above, RIM * last), roll(here, -RIM))
        leading = jnp.where(lane_tile == 0, roll(below, -RIM * last), roll(here, RIM))
        out = None
        for j in range(1, 5):
            up = roll(jnp.where(line >= j, here, following), -j, 0)
            down = roll(jnp.where(line < TILE - j, here, leading), j, 0)
            term = STENCIL[j - 1] * (up - down)
            out = term if out is None else out + term
        return out

    def across(value):
        along = [cross(value[f]) for f in range(fields)]
        forcing = (along[1], along[4], None, None, along[1])
        out = []
        for f in range(fields):
            total = flow_pack[0] * along[f]
            out.append(total if forcing[f] is None else total + forcing[f])
        return out

    def swapped(value):
        return jnp.where(rotor_side, roll(value, HALO), roll(value, -HALO))

    def sector_of(n, by, holder, sign):
        base = by + sign * offset_ref[n] - 1 + 2 * n_azim
        sector = base + lax.rem(holder - lax.rem(base, GROUP) + GROUP, GROUP)
        return lax.rem(sector, n_azim) // GROUP

    def facing_of(n, d):
        offset = offset_ref[n]
        stator_from = lax.rem(me - offset - 1 + d + 2 * n_azim, GROUP)
        rotor_from = lax.rem(me + offset - 1 + d + 2 * n_azim, GROUP)
        return stator_from, rotor_from

    def relay(e, n):
        for i, peer in enumerate(near_peers):
            near_copy(e, peer, peer, i).wait_recv()
        near_held[...] = near[e]

        def chosen(peer):
            by = high * GROUP + peer
            return jnp.where(
                rotor_side[None], near_held[sector_of(n, by, low, -1)], near_held[sector_of(n, by, low, 1)]
            )

        for i, peer in enumerate(far_peers):
            far_send[e, i] = chosen(peer)
            far_copy(e, low, peer, i).start()
        far[e, low] = chosen(low)

    def relay_params():
        for i, peer in enumerate(near_peers):
            par_copy(peer, peer, i).wait_recv()

        def chosen(peer, n):
            by = high * GROUP + peer
            return jnp.where(
                rotor_side, par[sector_of(n, by, low, -1)], par[sector_of(n, by, low, 1)]
            )

        for i, peer in enumerate(far_peers):
            for n in range(steps):
                par_send[i, n] = chosen(peer, n)
            pfar_copy(low, peer, i).start()
        for n in range(steps):
            par_far[low, n] = chosen(low, n)

    def ghosts(e, n, tap):
        for i, peer in enumerate(far_peers):
            far_copy(e, peer, peer, i).wait_recv()
        far_held[...] = far[e]
        spots = [facing_of(n, d) for d in range(3)]
        out = []
        for f in range(fields):
            facing = [jnp.where(rotor_side, far_held[s, f], far_held[r, f]) for s, r in spots]
            out.append(blend(facing[0], facing[1], facing[2], tap))
        return out

    def merge(e):
        for f in range(fields):
            value = tile[e, f]
            for group in range(cells * r_tiles):
                a, t = group // r_tiles, group % r_tiles
                spot = roll(value, low_lane - RIM * group)
                cur[e, f, a, pl.ds(TILE * (t + 1), TILE), :] = jnp.where(
                    at_interface, spot, raw[e, f, a, TILE * t : TILE * (t + 1), :]
                )

    def axial_slopes(e):
        for f in range(fields):
            block = cur[e, f, :, rows, :].reshape(cells * radial, lanes)
            slopes[f] = dot(block, deriv[...]).reshape(cells, radial, lanes)
        out = []
        for f in range(fields):
            plain = packed(lambda a, t: slopes[f, a, TILE * t : TILE * (t + 1), :])
            out.append(plain - cross(tile[e, f]))
        return out

    def rim_state(e, base, scale, along):
        out = []
        slope = []
        for f in range(fields):
            here = tile[e, f]
            slope.append((
                along[f],
                radial_slope(side[e, 2, f], here, side[e, 3, f]),
                azim_slope(side[e, 0, f], here, side[e, 1, f]),
            ))
        spread = slope[1][0] + slope[2][1] + slope[3][2]
        forcing = (spread, slope[4][0], slope[4][1], slope[4][2], spread)
        for f in range(fields):
            advect = flow_pack[0] * slope[f][0] + flow_pack[1] * slope[f][1] + flow_pack[2] * slope[f][2]
            out.append(tile[base, f] - scale * (advect + forcing[f]))
        return out

    def bulk_local(e, base, scale):
        on_rad(lambda: rad_copy(e, 1).wait_recv(), lambda: rad_copy(e, 0).wait_recv())
        cur[e, :, :, pl.ds(TILE - HALO, HALO), :] = rad_halo[e, 0]
        cur[e, :, :, pl.ds(TILE + radial, HALO), :] = rad_halo[e, 1]
        for a in range(cells):
            along = []
            for f in range(fields):
                rad_slope = None
                for j in range(4):
                    term = STENCIL[j] * (
                        cur[e, f, a, pl.ds(TILE + j + 1, radial), :]
                        - cur[e, f, a, pl.ds(TILE - j - 1, radial), :]
                    )
                    rad_slope = term if rad_slope is None else rad_slope + term
                along.append((slopes[f, a], rad_slope))
            spread = along[1][0] + along[2][1]
            forcing = (spread, along[4][0], along[4][1], None, spread)
            for f in range(fields):
                total = flow_ref[0] * along[f][0] + flow_ref[1] * along[f][1]
                if forcing[f] is not None:
                    total = total + forcing[f]
                slopes[f, a] = cur[base, f, a, rows, :] - scale * total

    def bulk_azim(e, scale, put):
        for side_no in range(2):
            for part in range(len(cuts) - 1):
                azim_copy(e, side_no, part).wait_recv()

        def cell_row(f, a):
            if a < 0:
                return azim_halo[e, 0, f, a + HALO]
            if a >= cells:
                return azim_halo[e, 1, f, a - cells]
            return cur[e, f, a, rows, :]

        for a in range(cells):
            along = []
            for f in range(fields):
                azim = None
                for j in range(4):
                    term = STENCIL[j] * (cell_row(f, a + j + 1) - cell_row(f, a - j - 1))
                    azim = term if azim is None else azim + term
                along.append(azim)
            forcing = (along[3], None, None, along[4], along[3])
            for f in range(fields):
                total = flow_ref[2] * along[f]
                if forcing[f] is not None:
                    total = total + forcing[f]
                put(f, a, slopes[f, a] - scale * total)

    def keep(e):
        def put(f, a, value):
            raw[e, f, a] = value

        return put

    def give(f, a, value):
        for t in range(r_tiles):
            part = slice(TILE * t, TILE * (t + 1))
            spot = roll(tile[evals, f], low_lane - RIM * (a * r_tiles + t))
            out_ref[f, a, part, :] = jnp.where(at_interface, spot, value[part])

    half_step = 0.5 * STEP_SIZE

    def advance(n, carry):
        e = 2 * n
        n_row = n + 1
        tap = taps(
            per_lane(stator_fraction, rotor_fraction), per_lane(stator_first(n), rotor_first(n))
        )
        merge(e)
        along = axial_slopes(e)
        relay(e, n)
        wait_sides(e)
        midway = rim_state(e, e, half_step, along)
        for f in range(fields):
            near[e + 1, high, f] = midway[f]
        send_near(e + 1)
        bulk_local(e, e, half_step)

        @pl.when(n == 0)
        def _():
            relay_params()

        bulk_azim(e, half_step, keep(e + 1))
        send_halos(e + 1, (0,))
        push = across(ghosts(e, n, tap))
        for f in range(fields):
            tile[e + 1, f] = midway[f] - half_step * push[f]
        send_sides(e + 1)

        merge(e + 1)
        along = axial_slopes(e + 1)

        relay(e + 1, n)
        send_halos(e + 1, (1,))
        bulk_local(e + 1, e, STEP_SIZE)
        @pl.when(n == 0)
        def _():
            for i, peer in enumerate(far_peers):
                pfar_copy(peer, peer, i).wait_recv()

        other = []
        for d in range(3):
            stator_from, rotor_from = facing_of(n, d)
            there = jnp.where(rotor_side, par_far[stator_from, n], par_far[rotor_from, n])
            there = swapped(there)
            fraction = jnp.broadcast_to(there[0:1], shape)
            first = jnp.zeros(shape, jnp.float32)
            for i in range(steps):
                first = jnp.where(n == i, jnp.broadcast_to(there[i + 1 : i + 2], shape), first)
            other.append(taps(fraction, first))
        back = taps(
            per_lane(rotor_fraction, stator_fraction), per_lane(rotor_first(n), stator_first(n))
        )
        twice = []
        for f in range(fields):
            before, here, after = side[e, 0, f], tile[e, f], side[e, 1, f]
            twice.append(blend(
                blend(before, before, here, other[0]),
                blend(before, here, after, other[1]),
                blend(here, after, after, other[2]),
                back,
            ))
        mutual = across(twice)

        wait_sides(e + 1)
        final = rim_state(e + 1, e, STEP_SIZE, along)
        ghost = ghosts(e + 1, n, tap)
        push = across([ghost[f] - half_step * mutual[f] for f in range(fields)])
        for f in range(fields):
            tile[e + 2, f] = final[f] - STEP_SIZE * push[f]

        @pl.when(n + 1 < steps)
        def _():
            for f in range(fields):
                near[e + 2, high, f] = tile[e + 2, f]
            send_near(e + 2)
            send_sides(e + 2)

        @pl.when(n + 1 < steps)
        def _():
            bulk_azim(e + 1, STEP_SIZE, keep(e + 2))
            send_halos(e + 2, range(2))

        @pl.when(n + 1 == steps)
        def _():
            bulk_azim(e + 1, STEP_SIZE, give)

        return carry

    lax.fori_loop(0, steps, advance, 0)
    def finish(e, carry):
        for i, peer in enumerate(near_peers):
            near_copy(e, high, peer, i).wait_send()
        for i, peer in enumerate(far_peers):
            far_copy(e, low, peer, i).wait_send()
        for side_no in range(2):
            for part in range(len(cuts) - 1):
                azim_copy(e, side_no, part).wait_send()
            side_copy(e, side_no).wait_send()

        def up():
            rad_copy(e, 0).wait_send()
            side_copy(e, 2).wait_send()

        def down():
            rad_copy(e, 1).wait_send()
            side_copy(e, 3).wait_send()

        on_rad(up, down)
        return carry

    lax.fori_loop(0, evals, finish, 0)
    for i, peer in enumerate(near_peers):
        par_copy(high, peer, i).wait_send()
    for i, peer in enumerate(far_peers):
        pfar_copy(low, peer, i).wait_send()


def solution(mesh):
    n_azim, n_rad = mesh.shape["azim"], mesh.shape["rad"]

    def shards(acoustic_state, mean_flow, sector_offset, cell_shift, stencil_start, interface_fraction):
        fields, cells, radial, lanes = acoustic_state.shape
        steps = sector_offset.shape[0]
        evals = 2 * steps
        n_high = n_azim // GROUP
        dims = (fields, cells, radial, lanes, steps, n_azim, n_rad)
        vmem = pl.BlockSpec(memory_space=pltpu.VMEM)
        f32 = jnp.float32
        dma = pltpu.SemaphoreType.DMA
        return pl.pallas_call(
            functools.partial(kernel, dims),
            out_shape=pltpu.VMEM(acoustic_state.shape, f32),
            in_specs=[pl.BlockSpec(memory_space=pl.ANY)] * 6,
            out_specs=vmem,
            scratch_shapes=[
                pltpu.VMEM(mean_flow.shape, f32),
                pltpu.SMEM(sector_offset.shape, jnp.int32),
                pltpu.SMEM(cell_shift.shape, jnp.int32),
                pltpu.SMEM(stencil_start.shape, jnp.int32),
                pltpu.SMEM(interface_fraction.shape, f32),
                dma((6,)),
                pltpu.VMEM((evals + 1, fields, cells, radial, lanes), f32),
                pltpu.VMEM((evals, fields, cells, radial + 2 * TILE, lanes), f32),
                pltpu.VMEM((evals, 2, fields, HALO, radial, lanes), f32),
                pltpu.VMEM((evals, 2, fields, cells, HALO, lanes), f32),
                pltpu.VMEM((evals, 2, fields, cells, HALO, lanes), f32),
                pltpu.VMEM((evals + 1, fields, TILE, lanes), f32),
                pltpu.VMEM((evals, 4, fields, TILE, lanes), f32),
                pltpu.VMEM((evals, n_high, fields, TILE, lanes), f32),
                pltpu.VMEM((evals, GROUP - 1, fields, TILE, lanes), f32),
                pltpu.VMEM((evals, GROUP, fields, TILE, lanes), f32),
                pltpu.VMEM((fields, cells, radial, lanes), f32),
                pltpu.VMEM((3, TILE, lanes), f32),
                pltpu.VMEM((lanes, lanes), f32),
                pltpu.VMEM((n_high, fields, TILE, lanes), f32),
                pltpu.VMEM((GROUP, fields, TILE, lanes), f32),
                pltpu.VMEM((n_high, TILE, lanes), f32),
                pltpu.VMEM((GROUP - 1, steps, TILE, lanes), f32),
                pltpu.VMEM((GROUP, steps, TILE, lanes), f32),
                dma((evals, n_high)), dma((evals, n_high)),
                dma((evals, GROUP)), dma((evals, GROUP)),
                dma((evals, 2, 2)), dma((evals, 2, 2)),
                dma((evals, 2)), dma((evals, 2)),
                dma((evals, 4)), dma((evals, 4)),
                dma((n_high,)), dma((n_high,)),
                dma((GROUP,)), dma((GROUP,)),
            ],
            compiler_params=pltpu.CompilerParams(collective_id=0, has_side_effects=True),
        )(acoustic_state, mean_flow, sector_offset, cell_shift, stencil_start, interface_fraction)

    return jax.shard_map(
        shards,
        mesh=mesh,
        in_specs=(
            P(None, "azim", "rad", None),
            P(None, "rad", None),
            P(),
            P(None, "azim"),
            P(None, "azim"),
            P(None, "azim"),
        ),
        out_specs=P(None, "azim", "rad", None),
        check_vma=False,
    )
```

```python
import functools

import jax
import jax.numpy as jnp
from jax import lax
from jax.experimental import pallas as pl
from jax.experimental.pallas import tpu as pltpu
from jax.sharding import PartitionSpec as P

STENCIL = (0.841570125482, -0.244678631765, 0.059463584768, -0.007650904064)
STEP_SIZE = 0.2
MESH = pl.DeviceIdType.MESH
HIGHEST = lax.Precision.HIGHEST
GROUP = 4
RIM = 8
TILE = 8
HALO = 4


def dot(a, b):
    return jnp.dot(a, b, precision=HIGHEST, preferred_element_type=jnp.float32)


def iota(shape, dim):
    return lax.broadcasted_iota(jnp.int32, shape, dim)


def kernel(
    dims,
    q_hbm, flow_hbm, offset_hbm, shift_hbm, start_hbm, fraction_hbm,
    out_ref,
    flow_ref, offset_ref, shift_ref, start_ref, fraction_ref, in_sem,
    raw, cur, azim_halo, rad_send, rad_halo, tile, side, near, far_send, far, slopes, flow_pack, deriv,
    near_held, far_held, par, par_send, par_far,
    near_ssem, near_rsem, far_ssem, far_rsem, azim_ssem, azim_rsem, rad_ssem, rad_rsem, side_ssem, side_rsem,
    par_ssem, par_rsem, pfar_ssem, pfar_rsem,
):
    fields, cells, radial, lanes, steps, n_azim, n_rad = dims
    evals = 2 * steps
    n_high = n_azim // GROUP
    middle = lanes // 2
    low_lane = middle - HALO
    r_tiles = radial // TILE
    span = RIM * r_tiles
    me = lax.axis_index("azim")
    rad = lax.axis_index("rad")
    high, low = me // GROUP, lax.rem(me, GROUP)
    left, right = lax.rem(me + n_azim - 1, n_azim), lax.rem(me + 1, n_azim)
    turn = 2 * (high // ((n_high + 1) // 2)) - 1
    near_peers = [lax.rem(high + turn * i + n_high, n_high) for i in range(1, n_high)]
    far_peers = [lax.rem(low + i, GROUP) for i in range(1, GROUP)]

    rows = pl.ds(TILE, radial)
    state_in = pltpu.make_async_copy(q_hbm, raw.at[0], in_sem.at[0])
    state_in.start()
    barrier = pltpu.get_barrier_semaphore()

    def greet(azim_to, rad_to):
        pl.semaphore_signal(barrier, inc=1, device_id=(azim_to, rad_to), device_id_type=MESH)

    greet(left, rad)
    greet(right, rad)
    for peer in near_peers:
        greet(peer * GROUP + low, rad)
    for peer in far_peers:
        greet(high * GROUP + peer, rad)

    @pl.when(rad > 0)
    def _():
        greet(me, rad - 1)

    @pl.when(rad < n_rad - 1)
    def _():
        greet(me, rad + 1)

    small_in = [
        pltpu.make_async_copy(source, target, in_sem.at[1 + i])
        for i, (source, target) in enumerate((
            (flow_hbm, flow_ref), (offset_hbm, offset_ref), (shift_hbm, shift_ref),
            (start_hbm, start_ref), (fraction_hbm, fraction_ref),
        ))
    ]
    for copy in small_in:
        copy.start()

    shape = (TILE, lanes)
    lane = iota(shape, 1)
    line = iota(shape, 0)
    lane_rim = lax.rem(lane, RIM)
    lane_group = lane // RIM
    rotor_side = lane_rim >= HALO
    lane_cell = lane // span
    lane_tile = lax.rem(lane_group, r_tiles)
    at_interface = (lane >= low_lane) & (lane < low_lane + RIM)

    def roll(value, turn, axis=1):
        turn = turn % value.shape[axis]
        return pltpu.roll(value, turn, axis) if turn else value

    def packed(piece_of):
        out = None
        for group in range(cells * r_tiles):
            piece = roll(piece_of(group // r_tiles, group % r_tiles), RIM * group - low_lane)
            out = piece if out is None else jnp.where(lane_group == group, piece, out)
        return out

    def near_copy(e, slot, peer, i):
        return pltpu.make_async_remote_copy(
            src_ref=near.at[e, high], dst_ref=near.at[e, slot],
            send_sem=near_ssem.at[e, i], recv_sem=near_rsem.at[e, slot],
            device_id=(peer * GROUP + low, rad), device_id_type=MESH,
        )

    def far_copy(e, slot, peer, i):
        return pltpu.make_async_remote_copy(
            src_ref=far_send.at[e, i], dst_ref=far.at[e, slot],
            send_sem=far_ssem.at[e, i], recv_sem=far_rsem.at[e, slot],
            device_id=(high * GROUP + peer, rad), device_id_type=MESH,
        )

    def par_copy(slot, peer, i):
        return pltpu.make_async_remote_copy(
            src_ref=par.at[high], dst_ref=par.at[slot],
            send_sem=par_ssem.at[i], recv_sem=par_rsem.at[slot],
            device_id=(peer * GROUP + low, rad), device_id_type=MESH,
        )

    def pfar_copy(slot, peer, i):
        return pltpu.make_async_remote_copy(
            src_ref=par_send.at[i], dst_ref=par_far.at[slot],
            send_sem=pfar_ssem.at[i], recv_sem=pfar_rsem.at[slot],
            device_id=(high * GROUP + peer, rad), device_id_type=MESH,
        )

    cuts = (0, 3, 5)

    def azim_copy(e, side_no, part):
        source = cells - HALO if side_no == 0 else 0
        some = pl.ds(cuts[part], cuts[part + 1] - cuts[part])
        return pltpu.make_async_remote_copy(
            src_ref=raw.at[e, some, pl.ds(source, HALO)], dst_ref=azim_halo.at[e, side_no, some],
            send_sem=azim_ssem.at[e, side_no, part], recv_sem=azim_rsem.at[e, side_no, part],
            device_id=(right if side_no == 0 else left, rad), device_id_type=MESH,
        )

    def rad_copy(e, side_no):
        return pltpu.make_async_remote_copy(
            src_ref=rad_send.at[e, side_no], dst_ref=rad_halo.at[e, side_no],
            send_sem=rad_ssem.at[e, side_no], recv_sem=rad_rsem.at[e, side_no],
            device_id=(me, rad + 1 if side_no == 0 else rad - 1), device_id_type=MESH,
        )

    def side_copy(e, slot):
        target = ((right, rad), (left, rad), (me, rad + 1), (me, rad - 1))[slot]
        return pltpu.make_async_remote_copy(
            src_ref=tile.at[e], dst_ref=side.at[e, slot],
            send_sem=side_ssem.at[e, slot], recv_sem=side_rsem.at[e, slot],
            device_id=target, device_id_type=MESH,
        )

    def on_rad(up, down):
        @pl.when(rad < n_rad - 1)
        def _():
            up()

        @pl.when(rad > 0)
        def _():
            down()

    def send_near(e):
        for i, peer in enumerate(near_peers):
            near_copy(e, high, peer, i).start()

    def send_sides(e):
        side_copy(e, 0).start()
        side_copy(e, 1).start()
        on_rad(lambda: side_copy(e, 2).start(), lambda: side_copy(e, 3).start())

    def wait_sides(e):
        on_rad(lambda: side_copy(e, 3).wait_recv(), lambda: side_copy(e, 2).wait_recv())
        side_copy(e, 0).wait_recv()
        side_copy(e, 1).wait_recv()

    def send_halos(e, which):
        for part in which:
            for side_no in range(2):
                azim_copy(e, side_no, part).start()
        if 0 not in which:
            return

        def up():
            rad_send[e, 0] = raw[e, :, :, pl.ds(radial - HALO, HALO), :]
            rad_copy(e, 0).start()

        def down():
            rad_send[e, 1] = raw[e, :, :, pl.ds(0, HALO), :]
            rad_copy(e, 1).start()

        on_rad(up, down)

    state_in.wait()
    for f in range(fields):
        first_tile = packed(lambda a, t: raw[0, f, a, TILE * t : TILE * (t + 1), :])
        tile[0, f] = first_tile
        near[0, high, f] = first_tile

    for copy in small_in:
        copy.wait()

    def per_lane(on_rotor, on_stator):
        out = jnp.zeros(shape, jnp.float32)
        for a in range(cells):
            out = jnp.where(lane_cell == a, jnp.where(rotor_side, on_rotor(a), on_stator(a)), out)
        return out

    def real(value):
        return value.astype(jnp.float32)

    def stator_first(n):
        return lambda a: real(shift_ref[n, a] + start_ref[0, a] - 1)

    def rotor_first(n):
        return lambda a: real(start_ref[1, a] - shift_ref[n, a] - 4)

    stator_fraction, rotor_fraction = (lambda a: fraction_ref[0, a]), (lambda a: fraction_ref[1, a])
    held = per_lane(rotor_fraction, stator_fraction)
    for n in range(steps):
        held = jnp.where(line == n + 1, per_lane(rotor_first(n), stator_first(n)), held)
    par[high] = held

    beside = jnp.where(rad > 0, 1, 0) + jnp.where(rad < n_rad - 1, 1, 0)
    pl.semaphore_wait(barrier, n_high - 1 + GROUP - 1 + 2 + beside)

    send_near(0)
    send_sides(0)
    send_halos(0, range(2))
    for i, peer in enumerate(near_peers):
        par_copy(high, peer, i).start()

    @pl.when(rad == 0)
    def _():
        for e in range(evals):
            rad_halo[e, 0] = jnp.zeros(rad_halo.shape[2:], jnp.float32)
            side[e, 2] = jnp.zeros(side.shape[2:], jnp.float32)

    @pl.when(rad == n_rad - 1)
    def _():
        for e in range(evals):
            rad_halo[e, 1] = jnp.zeros(rad_halo.shape[2:], jnp.float32)
            side[e, 3] = jnp.zeros(side.shape[2:], jnp.float32)

    row_no = iota((lanes, lanes), 0)
    col_no = iota((lanes, lanes), 1)
    axial = jnp.zeros((lanes, lanes), jnp.float32)
    for j in range(4):
        axial = jnp.where(row_no - col_no == j + 1, STENCIL[j], axial)
        axial = jnp.where(col_no - row_no == j + 1, -STENCIL[j], axial)
    deriv[...] = axial
    for i in range(3):
        flow_pack[i] = packed(lambda a, t: flow_ref[i, TILE * t : TILE * (t + 1), :])

    def taps(fraction, first):
        up_one, down_one, down_two = fraction + 1.0, fraction - 1.0, fraction - 2.0
        weights = (
            -fraction * down_one * down_two / 6.0,
            up_one * down_one * down_two / 2.0,
            -up_one * fraction * down_two / 2.0,
            up_one * fraction * down_one / 6.0,
        )
        out = []
        for delta in range(-HALO, HALO):
            tap = jnp.zeros(shape, jnp.float32)
            for m in range(4):
                tap = jnp.where(first == float(delta - m), weights[m], tap)
            out.append(tap)
        return out

    def shifted(before, here, after, delta):
        if delta < 0:
            here = jnp.where(lane_cell >= cells + delta, before, here)
        elif delta > 0:
            here = jnp.where(lane_cell < delta, after, here)
        return roll(here, -span * delta)

    def blend(before, here, after, tap):
        out = None
        for delta in range(-HALO, HALO):
            term = tap[delta + HALO] * shifted(before, here, after, delta)
            out = term if out is None else out + term
        return out

    ahead = [jnp.where((lane_rim < HALO) & (lane_rim + j + 1 >= HALO), STENCIL[j], 0.0) for j in range(4)]
    behind = [jnp.where((lane_rim >= HALO) & (lane_rim - j - 1 < HALO), STENCIL[j], 0.0) for j in range(4)]

    def cross(value):
        out = None
        for j in range(4):
            term = ahead[j] * roll(value, -(j + 1)) - behind[j] * roll(value, j + 1)
            out = term if out is None else out + term
        return out

    def azim_slope(before, here, after):
        out = None
        for j in range(4):
            term = STENCIL[j] * (
                shifted(before, here, after, j + 1) - shifted(before, here, after, -(j + 1))
            )
            out = term if out is None else out + term
        return out

    def radial_slope(below, here, above):
        last = r_tiles - 1
        following = jnp.where(lane_tile == last, roll(above, RIM * last), roll(here, -RIM))
        leading = jnp.where(lane_tile == 0, roll(below, -RIM * last), roll(here, RIM))
        out = None
        for j in range(1, 5):
            up = roll(jnp.where(line >= j, here, following), -j, 0)
            down = roll(jnp.where(line < TILE - j, here, leading), j, 0)
            term = STENCIL[j - 1] * (up - down)
            out = term if out is None else out + term
        return out

    def across(value):
        along = [cross(value[f]) for f in range(fields)]
        forcing = (along[1], along[4], None, None, along[1])
        out = []
        for f in range(fields):
            total = flow_pack[0] * along[f]
            out.append(total if forcing[f] is None else total + forcing[f])
        return out

    def swapped(value):
        return jnp.where(rotor_side, roll(value, HALO), roll(value, -HALO))

    def sector_of(n, by, holder, sign):
        base = by + sign * offset_ref[n] - 1 + 2 * n_azim
        sector = base + lax.rem(holder - lax.rem(base, GROUP) + GROUP, GROUP)
        return lax.rem(sector, n_azim) // GROUP

    def facing_of(n, d):
        offset = offset_ref[n]
        stator_from = lax.rem(me - offset - 1 + d + 2 * n_azim, GROUP)
        rotor_from = lax.rem(me + offset - 1 + d + 2 * n_azim, GROUP)
        return stator_from, rotor_from

    def relay(e, n):
        for i, peer in enumerate(near_peers):
            near_copy(e, peer, peer, i).wait_recv()
        near_held[...] = near[e]

        def chosen(peer):
            by = high * GROUP + peer
            return jnp.where(
                rotor_side[None], near_held[sector_of(n, by, low, -1)], near_held[sector_of(n, by, low, 1)]
            )

        for i, peer in enumerate(far_peers):
            far_send[e, i] = chosen(peer)
            far_copy(e, low, peer, i).start()
        far[e, low] = chosen(low)

    def relay_params():
        for i, peer in enumerate(near_peers):
            par_copy(peer, peer, i).wait_recv()

        def chosen(peer, n):
            by = high * GROUP + peer
            return jnp.where(
                rotor_side, par[sector_of(n, by, low, -1)], par[sector_of(n, by, low, 1)]
            )

        for i, peer in enumerate(far_peers):
            for n in range(steps):
                par_send[i, n] = chosen(peer, n)
            pfar_copy(low, peer, i).start()
        for n in range(steps):
            par_far[low, n] = chosen(low, n)

    def ghosts(e, n, tap):
        for i, peer in enumerate(far_peers):
            far_copy(e, peer, peer, i).wait_recv()
        far_held[...] = far[e]
        spots = [facing_of(n, d) for d in range(3)]
        out = []
        for f in range(fields):
            facing = [jnp.where(rotor_side, far_held[s, f], far_held[r, f]) for s, r in spots]
            out.append(blend(facing[0], facing[1], facing[2], tap))
        return out

    def merge(e):
        for f in range(fields):
            value = tile[e, f]
            for group in range(cells * r_tiles):
                a, t = group // r_tiles, group % r_tiles
                spot = roll(value, low_lane - RIM * group)
                cur[e, f, a, pl.ds(TILE * (t + 1), TILE), :] = jnp.where(
                    at_interface, spot, raw[e, f, a, TILE * t : TILE * (t + 1), :]
                )

    def axial_slopes(e):
        for f in range(fields):
            block = cur[e, f, :, rows, :].reshape(cells * radial, lanes)
            slopes[f] = dot(block, deriv[...]).reshape(cells, radial, lanes)
        out = []
        for f in range(fields):
            plain = packed(lambda a, t: slopes[f, a, TILE * t : TILE * (t + 1), :])
            out.append(plain - cross(tile[e, f]))
        return out

    def rim_state(e, base, scale, along):
        out = []
        slope = []
        for f in range(fields):
            here = tile[e, f]
            slope.append((
                along[f],
                radial_slope(side[e, 2, f], here, side[e, 3, f]),
                azim_slope(side[e, 0, f], here, side[e, 1, f]),
            ))
        spread = slope[1][0] + slope[2][1] + slope[3][2]
        forcing = (spread, slope[4][0], slope[4][1], slope[4][2], spread)
        for f in range(fields):
            advect = flow_pack[0] * slope[f][0] + flow_pack[1] * slope[f][1] + flow_pack[2] * slope[f][2]
            out.append(tile[base, f] - scale * (advect + forcing[f]))
        return out

    def bulk_local(e, base, scale):
        on_rad(lambda: rad_copy(e, 1).wait_recv(), lambda: rad_copy(e, 0).wait_recv())
        cur[e, :, :, pl.ds(TILE - HALO, HALO), :] = rad_halo[e, 0]
        cur[e, :, :, pl.ds(TILE + radial, HALO), :] = rad_halo[e, 1]
        for a in range(cells):
            along = []
            for f in range(fields):
                rad_slope = None
                for j in range(4):
                    term = STENCIL[j] * (
                        cur[e, f, a, pl.ds(TILE + j + 1, radial), :]
                        - cur[e, f, a, pl.ds(TILE - j - 1, radial), :]
                    )
                    rad_slope = term if rad_slope is None else rad_slope + term
                along.append((slopes[f, a], rad_slope))
            spread = along[1][0] + along[2][1]
            forcing = (spread, along[4][0], along[4][1], None, spread)
            for f in range(fields):
                total = flow_ref[0] * along[f][0] + flow_ref[1] * along[f][1]
                if forcing[f] is not None:
                    total = total + forcing[f]
                slopes[f, a] = cur[base, f, a, rows, :] - scale * total

    def bulk_azim(e, scale, put):
        for side_no in range(2):
            for part in range(len(cuts) - 1):
                azim_copy(e, side_no, part).wait_recv()

        def cell_row(f, a):
            if a < 0:
                return azim_halo[e, 0, f, a + HALO]
            if a >= cells:
                return azim_halo[e, 1, f, a - cells]
            return cur[e, f, a, rows, :]

        for a in range(cells):
            along = []
            for f in range(fields):
                azim = None
                for j in range(4):
                    term = STENCIL[j] * (cell_row(f, a + j + 1) - cell_row(f, a - j - 1))
                    azim = term if azim is None else azim + term
                along.append(azim)
            forcing = (along[3], None, None, along[4], along[3])
            for f in range(fields):
                total = flow_ref[2] * along[f]
                if forcing[f] is not None:
                    total = total + forcing[f]
                put(f, a, slopes[f, a] - scale * total)

    def keep(e):
        def put(f, a, value):
            raw[e, f, a] = value

        return put

    def give(f, a, value):
        for t in range(r_tiles):
            part = slice(TILE * t, TILE * (t + 1))
            spot = roll(tile[evals, f], low_lane - RIM * (a * r_tiles + t))
            out_ref[f, a, part, :] = jnp.where(at_interface, spot, value[part])

    half_step = 0.5 * STEP_SIZE

    def advance(n, carry):
        e = 2 * n
        n_row = n + 1
        tap = taps(
            per_lane(stator_fraction, rotor_fraction), per_lane(stator_first(n), rotor_first(n))
        )
        merge(e)
        along = axial_slopes(e)
        relay(e, n)
        wait_sides(e)
        midway = rim_state(e, e, half_step, along)
        for f in range(fields):
            near[e + 1, high, f] = midway[f]
        send_near(e + 1)
        bulk_local(e, e, half_step)

        @pl.when(n == 0)
        def _():
            relay_params()

        bulk_azim(e, half_step, keep(e + 1))
        send_halos(e + 1, (0,))
        push = across(ghosts(e, n, tap))
        for f in range(fields):
            tile[e + 1, f] = midway[f] - half_step * push[f]
        send_sides(e + 1)

        merge(e + 1)
        along = axial_slopes(e + 1)

        relay(e + 1, n)
        send_halos(e + 1, (1,))
        bulk_local(e + 1, e, STEP_SIZE)
        @pl.when(n == 0)
        def _():
            for i, peer in enumerate(far_peers):
                pfar_copy(peer, peer, i).wait_recv()

        other = []
        for d in range(3):
            stator_from, rotor_from = facing_of(n, d)
            there = jnp.where(rotor_side, par_far[stator_from, n], par_far[rotor_from, n])
            there = swapped(there)
            fraction = jnp.broadcast_to(there[0:1], shape)
            first = jnp.zeros(shape, jnp.float32)
            for i in range(steps):
                first = jnp.where(n == i, jnp.broadcast_to(there[i + 1 : i + 2], shape), first)
            other.append(taps(fraction, first))
        back = taps(
            per_lane(rotor_fraction, stator_fraction), per_lane(rotor_first(n), stator_first(n))
        )
        twice = []
        for f in range(fields):
            before, here, after = side[e, 0, f], tile[e, f], side[e, 1, f]
            twice.append(blend(
                blend(before, before, here, other[0]),
                blend(before, here, after, other[1]),
                blend(here, after, after, other[2]),
                back,
            ))
        mutual = across(twice)

        wait_sides(e + 1)
        final = rim_state(e + 1, e, STEP_SIZE, along)
        ghost = ghosts(e + 1, n, tap)
        push = across([ghost[f] - half_step * mutual[f] for f in range(fields)])
        for f in range(fields):
            tile[e + 2, f] = final[f] - STEP_SIZE * push[f]

        @pl.when(n + 1 < steps)
        def _():
            for f in range(fields):
                near[e + 2, high, f] = tile[e + 2, f]
            send_near(e + 2)
            send_sides(e + 2)

        @pl.when(n + 1 < steps)
        def _():
            bulk_azim(e + 1, STEP_SIZE, keep(e + 2))
            send_halos(e + 2, range(2))

        @pl.when(n + 1 == steps)
        def _():
            bulk_azim(e + 1, STEP_SIZE, give)

        return carry

    lax.fori_loop(0, steps, advance, 0)
    def finish(e, carry):
        for i, peer in enumerate(near_peers):
            near_copy(e, high, peer, i).wait_send()
        for i, peer in enumerate(far_peers):
            far_copy(e, low, peer, i).wait_send()
        for side_no in range(2):
            for part in range(len(cuts) - 1):
                azim_copy(e, side_no, part).wait_send()
            side_copy(e, side_no).wait_send()

        def up():
            rad_copy(e, 0).wait_send()
            side_copy(e, 2).wait_send()

        def down():
            rad_copy(e, 1).wait_send()
            side_copy(e, 3).wait_send()

        on_rad(up, down)
        return carry

    lax.fori_loop(0, evals, finish, 0)
    for i, peer in enumerate(near_peers):
        par_copy(high, peer, i).wait_send()
    for i, peer in enumerate(far_peers):
        pfar_copy(low, peer, i).wait_send()


def solution(mesh):
    n_azim, n_rad = mesh.shape["azim"], mesh.shape["rad"]

    def shards(acoustic_state, mean_flow, sector_offset, cell_shift, stencil_start, interface_fraction):
        fields, cells, radial, lanes = acoustic_state.shape
        steps = sector_offset.shape[0]
        evals = 2 * steps
        n_high = n_azim // GROUP
        dims = (fields, cells, radial, lanes, steps, n_azim, n_rad)
        vmem = pl.BlockSpec(memory_space=pltpu.VMEM)
        f32 = jnp.float32
        dma = pltpu.SemaphoreType.DMA
        return pl.pallas_call(
            functools.partial(kernel, dims),
            out_shape=pltpu.VMEM(acoustic_state.shape, f32),
            in_specs=[pl.BlockSpec(memory_space=pl.ANY)] * 6,
            out_specs=vmem,
            scratch_shapes=[
                pltpu.VMEM(mean_flow.shape, f32),
                pltpu.SMEM(sector_offset.shape, jnp.int32),
                pltpu.SMEM(cell_shift.shape, jnp.int32),
                pltpu.SMEM(stencil_start.shape, jnp.int32),
                pltpu.SMEM(interface_fraction.shape, f32),
                dma((6,)),
                pltpu.VMEM((evals + 1, fields, cells, radial, lanes), f32),
                pltpu.VMEM((evals, fields, cells, radial + 2 * TILE, lanes), f32),
                pltpu.VMEM((evals, 2, fields, HALO, radial, lanes), f32),
                pltpu.VMEM((evals, 2, fields, cells, HALO, lanes), f32),
                pltpu.VMEM((evals, 2, fields, cells, HALO, lanes), f32),
                pltpu.VMEM((evals + 1, fields, TILE, lanes), f32),
                pltpu.VMEM((evals, 4, fields, TILE, lanes), f32),
                pltpu.VMEM((evals, n_high, fields, TILE, lanes), f32),
                pltpu.VMEM((evals, GROUP - 1, fields, TILE, lanes), f32),
                pltpu.VMEM((evals, GROUP, fields, TILE, lanes), f32),
                pltpu.VMEM((fields, cells, radial, lanes), f32),
                pltpu.VMEM((3, TILE, lanes), f32),
                pltpu.VMEM((lanes, lanes), f32),
                pltpu.VMEM((n_high, fields, TILE, lanes), f32),
                pltpu.VMEM((GROUP, fields, TILE, lanes), f32),
                pltpu.VMEM((n_high, TILE, lanes), f32),
                pltpu.VMEM((GROUP - 1, steps, TILE, lanes), f32),
                pltpu.VMEM((GROUP, steps, TILE, lanes), f32),
                dma((evals, n_high)), dma((evals, n_high)),
                dma((evals, GROUP)), dma((evals, GROUP)),
                dma((evals, 2, 2)), dma((evals, 2, 2)),
                dma((evals, 2)), dma((evals, 2)),
                dma((evals, 4)), dma((evals, 4)),
                dma((n_high,)), dma((n_high,)),
                dma((GROUP,)), dma((GROUP,)),
            ],
            compiler_params=pltpu.CompilerParams(collective_id=0, has_side_effects=True),
        )(acoustic_state, mean_flow, sector_offset, cell_shift, stencil_start, interface_fraction)

    return jax.shard_map(
        shards,
        mesh=mesh,
        in_specs=(
            P(None, "azim", "rad", None),
            P(None, "rad", None),
            P(),
            P(None, "azim"),
            P(None, "azim"),
            P(None, "azim"),
        ),
        out_specs=P(None, "azim", "rad", None),
        check_vma=False,
    )
```
